32 devices in a mesh: batch: 1 (over z), w: 4 (over y), h: 8 (over x, core).
Axes of the slice: x: 4, y: 4, z: 1, core: 2. Of those that a mesh axis runs over, the one named last changes fastest.
The devices are a block of a 4x4x8 slice.
Arguments:
- image: bfloat16 [256, 2048, 32, 1], P('batch', 'h', 'w')
- down_w1: bfloat16 [3, 3, 1, 64], replicated
- down_v1: float32 [3, 64], replicated
- refine_w1: bfloat16 [3, 3, 64, 64], replicated
- refine_v1: float32 [3, 64], replicated
- down_w2: bfloat16 [3, 3, 64, 128], replicated
- down_v2: float32 [3, 128], replicated
- refine_w2: bfloat16 [3, 3, 128, 128], replicated
- refine_v2: float32 [3, 128], replicated
- down_w3: bfloat16 [3, 3, 128, 256], replicated
- down_v3: float32 [3, 256], replicated
- refine_w3: bfloat16 [3, 3, 256, 256], replicated
- refine_v3: float32 [3, 256], replicated
Outputs:
- output: bfloat16 [256, 256, 4, 256], P('batch', 'h', 'w')
All inputs are finite; a program needn't handle non-finite values.
Results may differ from the reference program's by a relative error of at most 0.00374919.
Values are sent between devices in bfloat16 or wider.
A program may use at most 768 MiB of HBM per device.

```python
import jax
import jax.numpy as jnp
from jax import lax

IMAGES = 256
IMG_HEIGHT = 2048
IMG_WIDTH = 32
CHAN_IN = 1
CHAN_ONE = 64
GROUPS = 8
NORM_EPS = 1e-5


def draw_affine(key, channels):
    bias_key, scale_key, shift_key = jax.random.split(key, 3)
    bias = 0.5 * jax.random.normal(bias_key, (channels,), jnp.float32)
    scale = 1.0 + 0.3 * jax.random.normal(scale_key, (channels,), jnp.float32)
    shift = 0.3 * jax.random.normal(shift_key, (channels,), jnp.float32)
    return jnp.stack([bias, scale, shift])


def setup_inputs(seed: int = 0, part: int = 0) -> dict:
    shared_key, image_root = jax.random.split(jax.random.key(seed))
    image_key = jax.random.fold_in(image_root, part)
    noise_key, slope_key, level_key = jax.random.split(image_key, 3)
    noise = jax.random.normal(noise_key, (IMAGES, IMG_HEIGHT, IMG_WIDTH, CHAN_IN), jnp.float32)
    slopes = jax.random.normal(slope_key, (2, IMAGES, 1, 1, CHAN_IN), jnp.float32)
    levels = 0.5 * jax.random.normal(level_key, (IMAGES, 1, 1, CHAN_IN), jnp.float32)
    row_pos = (jnp.arange(IMG_HEIGHT, dtype=jnp.float32) + 0.5) * (2.0 / IMG_HEIGHT) - 1.0
    col_pos = (jnp.arange(IMG_WIDTH, dtype=jnp.float32) + 0.5) * (2.0 / IMG_WIDTH) - 1.0
    ramp = slopes[0] * row_pos[:, None, None] + slopes[1] * col_pos[:, None]
    image = (noise + 1.5 * ramp + levels).astype(jnp.bfloat16)
    widths = [CHAN_IN, CHAN_ONE, 2 * CHAN_ONE, 4 * CHAN_ONE]
    weight_keys = jax.random.split(shared_key, 12)
    inputs = {"image": image}
    for stage in range(3):
        chan_prev = widths[stage]
        chan_next = widths[stage + 1]
        down_w = jax.random.normal(weight_keys[4 * stage], (3, 3, chan_prev, chan_next), jnp.float32) * (9 * chan_prev) ** -0.5
        refine_w = jax.random.normal(weight_keys[4 * stage + 2], (3, 3, chan_next, chan_next), jnp.float32) * (9 * chan_next) ** -0.5
        inputs["down_w" + str(stage + 1)] = down_w.astype(jnp.bfloat16)
        inputs["down_v" + str(stage + 1)] = draw_affine(weight_keys[4 * stage + 1], chan_next)
        inputs["refine_w" + str(stage + 1)] = refine_w.astype(jnp.bfloat16)
        inputs["refine_v" + str(stage + 1)] = draw_affine(weight_keys[4 * stage + 3], chan_next)
    return inputs


def conv_norm(inputs, kernel, affine, stride):
    summed = lax.conv_general_dilated(inputs.astype(jnp.float32), kernel.astype(jnp.float32), (stride, stride), ((1, 1), (1, 1)), dimension_numbers=("NHWC", "HWIO", "NHWC")) + affine[0]
    out_shape = summed.shape
    grouped = summed.reshape(out_shape[0], out_shape[1], out_shape[2], GROUPS, out_shape[3] // GROUPS)
    grp_mean = jnp.mean(grouped, axis=(1, 2, 4), keepdims=True)
    centered = grouped - grp_mean
    grp_var = jnp.mean(jnp.square(centered), axis=(1, 2, 4), keepdims=True)
    normed = (centered * lax.rsqrt(grp_var + NORM_EPS)).reshape(out_shape)
    return jax.nn.relu(normed * affine[1] + affine[2]).astype(jnp.bfloat16)


def reference(image, down_w1, down_v1, refine_w1, refine_v1, down_w2, down_v2, refine_w2, refine_v2, down_w3, down_v3, refine_w3, refine_v3):
    stages = ((down_w1, down_v1, refine_w1, refine_v1), (down_w2, down_v2, refine_w2, refine_v2), (down_w3, down_v3, refine_w3, refine_v3))

    def one_image(single):
        current = single[None]
        for down_w, down_v, refine_w, refine_v in stages:
            current = conv_norm(current, down_w, down_v, 2)
            current = conv_norm(current, refine_w, refine_v, 1)
        return current[0]

    return lax.map(one_image, image)
```

```python
import jax
import jax.numpy as jnp
from jax import lax
from jax.sharding import PartitionSpec as P

NORM_GROUPS = 8
NORM_EPS = 1e-5


def conv_norm(inputs, kernel, affine, stride):
    pads = ((1, 0), (1, 0)) if stride == 2 else ((1, 1), (1, 1))
    summed = lax.conv_general_dilated(inputs, kernel, (stride, stride), pads, dimension_numbers=("NHWC", "HWIO", "NHWC"), preferred_element_type=jnp.float32) + affine[0]
    out_shape = summed.shape
    per_group = out_shape[3] // NORM_GROUPS
    pixel_count = out_shape[1] * out_shape[2] * per_group
    totals = jnp.stack([jnp.sum(summed, axis=(1, 2)), jnp.sum(jnp.square(summed), axis=(1, 2))])
    totals = jnp.sum(totals.reshape(2, out_shape[0], NORM_GROUPS, per_group), axis=3)
    grp_mean = totals[0] / pixel_count
    grp_var = jnp.maximum(totals[1] / pixel_count - jnp.square(grp_mean), 0.0)
    inv_std = lax.rsqrt(grp_var + NORM_EPS)
    chan_scale = jnp.repeat(inv_std, per_group, axis=1) * affine[1]
    chan_shift = affine[2] - jnp.repeat(grp_mean * inv_std, per_group, axis=1) * affine[1]
    return jax.nn.relu(summed * chan_scale[:, None, None, :] + chan_shift[:, None, None, :]).astype(jnp.bfloat16)


def solution(mesh):
    act_spec = P("batch", "h", "w")

    def local_forward(tile, *params):
        current = lax.all_to_all(tile, "h", 0, 1, tiled=True)
        current = lax.all_to_all(current, "w", 0, 2, tiled=True)
        for stage in range(3):
            down_w, down_v, refine_w, refine_v = params[4 * stage:4 * stage + 4]
            current = conv_norm(current, down_w, down_v, 2)
            current = conv_norm(current, refine_w, refine_v, 1)
        current = lax.all_to_all(current, "w", 2, 0, tiled=True)
        return lax.all_to_all(current, "h", 1, 0, tiled=True)

    return jax.shard_map(local_forward, mesh=mesh, in_specs=(act_spec,) + (P(),) * 12, out_specs=act_spec, check_vma=False)
```

```python
import functools

import jax
import jax.numpy as jnp
from jax import lax
from jax.experimental import pallas as pl
from jax.experimental.pallas import tpu as pltpu
from jax.sharding import PartitionSpec as P

NORM_GROUPS = 8
NORM_EPS = 1e-5
F32 = jnp.float32
BF16 = jnp.bfloat16
LANES = 128
STRIPS = 16


def iota(shape, dim):
    return lax.broadcasted_iota(jnp.int32, shape, dim)


def div(value, by):
    return lax.div(value, jnp.int32(by))


def rem(value, by):
    return lax.rem(value, jnp.int32(by))


def blend(pieces, rows, cols):
    return jnp.concatenate([jnp.zeros((rows, cols), BF16) if piece is None else piece for piece in pieces], axis=1)


def tap(ref, depth, row, col):
    if 0 <= row < 3 and 0 <= col < 3:
        return ref[pl.ds((3 * row + col) * depth, depth), :]
    return None


def build_weights(w1_ref, r1_ref, d2_ref, r2_ref, m1, m2, m3, m4, cols):
    taps = w1_ref[...].astype(F32)
    taps = jnp.concatenate([taps] * 4, axis=1)
    shape = (2 * LANES, 2 * LANES)
    k, n = iota(shape, 0), iota(shape, 1)
    kk = rem(k, LANES)
    row = 4 * (div(k, LANES) - 1) + rem(div(kk, 8), 4)
    col = 8 * div(kk, 32) + rem(kk, 8)
    d_row = row - 2 * div(n, LANES) + 1
    half = rem(div(n, 64), 2)
    row_ok = (d_row >= 0) & (d_row < 3)

    def one_block(block, _):
        col_out = 2 * block - 1 + half
        d_col = col - 2 * col_out + 1
        good = row_ok & (d_col >= 0) & (d_col < 3) & (col_out >= 0) & (col_out < cols // 2)
        code = jnp.where(good, 3 * d_row + d_col, -1)
        total = jnp.zeros(shape, F32)
        for index in range(9):
            total = jnp.where(code == index, taps[index:index + 1], total)
        m1[block] = total.astype(BF16)
        return 0

    lax.fori_loop(0, m1.shape[0], one_block, 0)
    for t in range(4):
        for q in range(4):
            m2[pl.ds((4 * t + q) * 64, 64), :] = blend([tap(r1_ref, 64, t - r, q - g) for r in range(2) for g in range(2)], 64, 64)
    for t in range(3):
        for q in range(6):
            m3[pl.ds((6 * t + q) * 64, 64), :] = blend([tap(d2_ref, 64, t, q - 1 - 2 * g) for g in range(2)], 64, LANES)
    for t in range(3):
        for q in range(4):
            m4[pl.ds((4 * t + q) * LANES, LANES), :] = blend([tap(r2_ref, LANES, t, q - g) for g in range(2)], LANES, LANES)


def group_matrix(period, group):
    shape = (LANES, LANES)
    return jnp.where(div(rem(iota(shape, 0), period), group) == div(rem(iota(shape, 1), period), group), 1.0, 0.0).astype(F32)


def down_strip(row):
    return jnp.where(iota(row.shape, 0) == 0, 0.0, pltpu.roll(row, 1, 0))


def up_strip(row):
    return jnp.where(iota(row.shape, 0) == STRIPS - 1, 0.0, pltpu.roll(row, STRIPS - 1, 0))


def coefficients(sums, squares, folds, gamma, beta, count):
    both = jnp.concatenate([sums, squares], axis=0)
    both = jnp.dot(both, folds, preferred_element_type=F32, precision=lax.Precision.HIGHEST)
    total = jnp.sum(both[:STRIPS], axis=0, keepdims=True)
    total_sq = jnp.sum(both[STRIPS:], axis=0, keepdims=True)
    mean = total / count
    var = jnp.maximum(total_sq / count - jnp.square(mean), 0.0)
    inv = lax.rsqrt(var + NORM_EPS)
    scale = inv * gamma
    return scale, beta - mean * scale


class Stream:
    def __init__(self, mats, affines, acc, x, y1, z1, y2, z2, y3, out, cols):
        self.mats, self.affines = mats, affines
        self.acc, self.x, self.y1, self.z1, self.y2, self.z2, self.y3, self.out = acc, x, y1, z1, y2, z2, y3, out
        self.cols = cols
        self.q = x.shape[0] - 1
        self.r2 = y2.shape[1] - 2
        self.r3 = y3.shape[2] - 2
        self.sums = None
        self.squares = None

    def lhs(self, parts):
        parts = [part.reshape(part.shape[0] * STRIPS, LANES) for part in parts]
        return jnp.concatenate(parts, axis=1)

    def finish(self, summed, bias, first, second):
        rows = summed.shape[0]
        summed = summed + bias
        cube = summed.reshape(rows // STRIPS, STRIPS, 2 * LANES)
        sums, squares = jnp.sum(cube, axis=0), jnp.sum(cube * cube, axis=0)
        self.sums = sums if self.sums is None else self.sums + sums
        self.squares = squares if self.squares is None else self.squares + squares
        self.acc[first, 0:rows] = summed[:, :LANES]
        self.acc[second, 0:rows] = summed[:, LANES:]

    def two(self, row):
        return jnp.concatenate([row, row], axis=1)

    def conv1(self):
        affine = self.affines[0]
        lane = iota((1, LANES), 1)
        blocks = self.mats[0].shape[0]
        bias = self.two(affine[0:1])

        def piece(block):
            own = bias
            if block == 0:
                own = self.two(jnp.where(lane < 64, 0.0, affine[0:1]))
            elif block == blocks - 1:
                own = self.two(jnp.where(lane < 64, affine[0:1], 0.0))
            left = self.lhs([self.x[0:self.q], self.x[1:self.q + 1]])
            self.finish(jnp.dot(left, self.mats[0][block], preferred_element_type=F32), own, 2 * block, 2 * block + 1)

        return [functools.partial(piece, block) for block in range(blocks)]

    def conv2(self):
        bias, q = self.two(self.affines[1][0:1]), self.q

        def piece(block):
            parts = []
            for parity, start in ((1, 0), (0, 1), (1, 1), (0, 2)):
                for near in range(2):
                    parts.append(self.y1[block + near, parity, start:start + q])
            self.finish(jnp.dot(self.lhs(parts), self.mats[1][...], preferred_element_type=F32), bias, 2 * block, 2 * block + 1)

        return [functools.partial(piece, block) for block in range(self.cols // 4)]

    def conv3(self):
        bias, q = self.two(self.affines[2][0:1]), self.q

        def piece(block):
            parts = []
            for parity, start in ((1, 0), (0, 1), (1, 1)):
                for near in range(3):
                    parts.append(self.z1[2 * block + near, parity, start:start + q])
            self.finish(jnp.dot(self.lhs(parts), self.mats[2][...], preferred_element_type=F32), bias, 2 * block, 2 * block + 1)

        return [functools.partial(piece, block) for block in range(self.cols // 8)]

    def conv4(self):
        bias = self.two(self.affines[3][0:1])

        def piece(block):
            parts = []
            for start in range(3):
                for near in range(4):
                    parts.append(self.y2[2 * block + near, start:start + self.r2])
            self.finish(jnp.dot(self.lhs(parts), self.mats[3][...], preferred_element_type=F32), bias, 2 * block, 2 * block + 1)

        return [functools.partial(piece, block) for block in range(self.cols // 8)]

    def conv5(self):
        bias = self.affines[4][0:1]

        def piece(col):
            parts = []
            for parity, start in ((1, 0), (0, 1), (1, 1)):
                for near in range(3):
                    parts.append(self.z2[2 * col + near, parity, start:start + self.r3])
            self.finish(jnp.dot(self.lhs(parts), self.mats[4][...], preferred_element_type=F32), bias, 2 * col, 2 * col + 1)

        return [functools.partial(piece, col) for col in range(self.cols // 8)]

    def conv6(self):
        bias = self.affines[5][0:1]

        def piece(col):
            parts = []
            for start in range(3):
                for near in range(3):
                    for half in range(2):
                        parts.append(self.y3[col + near, half, start:start + self.r3])
            self.finish(jnp.dot(self.lhs(parts), self.mats[5][...], preferred_element_type=F32), bias, 2 * col, 2 * col + 1)

        return [functools.partial(piece, col) for col in range(self.cols // 8)]

    def stats(self, layer):
        affine = self.affines[layer]
        period, group = ((64, 8), (LANES, 16), (LANES, 32))[layer // 2]
        folds = group_matrix(period, group)
        height = 1
        rows = (2 * self.q, self.r2, self.r3)[layer // 2]
        width = self.cols >> (layer // 2 + 1)
        count = float(height * rows * STRIPS * width * group)
        sums, squares = self.sums, self.squares
        self.sums = self.squares = None
        if layer < 4:
            sums, squares = sums[:, :LANES] + sums[:, LANES:], squares[:, :LANES] + squares[:, LANES:]
            self.scale, self.shift = coefficients(sums, squares, folds, affine[1:2], affine[2:3], count)
        else:
            pairs = [coefficients(sums[:, lo:lo + LANES], squares[:, lo:lo + LANES], folds, affine[1:2, lo:lo + LANES], affine[2:3, lo:lo + LANES], count) for lo in (0, LANES)]
            self.scale, self.shift = [pair[0] for pair in pairs], [pair[1] for pair in pairs]

    def apply(self, block, rows, scale, shift):
        cube = jnp.maximum(self.acc[block, 0:rows * STRIPS] * scale + shift, 0.0)
        return cube.reshape(rows, STRIPS, LANES)

    def norm1(self):
        lane, q = iota((1, LANES), 1), self.q
        blocks = self.mats[0].shape[0]

        def piece(block, parity):
            scale, shift = self.scale, self.shift
            if block == 0:
                scale, shift = jnp.where(lane < 64, 0.0, scale), jnp.where(lane < 64, 0.0, shift)
            elif block == blocks - 1:
                scale, shift = jnp.where(lane < 64, scale, 0.0), jnp.where(lane < 64, shift, 0.0)
            cube = self.apply(2 * block + parity, q, scale, shift)
            self.y1[block, parity, 1:q + 1] = cube.astype(BF16)
            if parity:
                self.y1[block, 1, 0] = down_strip(cube[q - 1]).astype(BF16)
            else:
                self.y1[block, 0, q + 1] = up_strip(cube[0]).astype(BF16)

        return [functools.partial(piece, block, parity) for block in range(blocks) for parity in range(2)]

    def norm2(self):
        q = self.q

        def piece(block, parity):
            cube = self.apply(2 * block + parity, q, self.scale, self.shift)
            self.z1[block + 1, parity, 1:q + 1] = cube.astype(BF16)
            if parity:
                self.z1[block + 1, 1, 0] = down_strip(cube[q - 1]).astype(BF16)

        return [functools.partial(piece, block, parity) for block in range(self.cols // 4) for parity in range(2)]

    def norm3(self):
        rows = self.r2

        def piece(col):
            cube = self.apply(col, rows, self.scale, self.shift)
            self.y2[col + 1, 1:rows + 1] = cube.astype(BF16)
            self.y2[col + 1, 0] = down_strip(cube[rows - 1]).astype(BF16)
            self.y2[col + 1, rows + 1] = up_strip(cube[0]).astype(BF16)

        return [functools.partial(piece, col) for col in range(self.cols // 4)]

    def norm4(self):
        rows = self.r3

        def piece(col):
            cube = self.apply(col, 2 * rows, self.scale, self.shift).reshape(rows, 2, STRIPS, LANES)
            self.z2[col + 1, 0, 1:rows + 1] = cube[:, 0].astype(BF16)
            self.z2[col + 1, 1, 1:rows + 1] = cube[:, 1].astype(BF16)
            self.z2[col + 1, 1, 0] = down_strip(cube[rows - 1, 1]).astype(BF16)

        return [functools.partial(piece, col) for col in range(self.cols // 4)]

    def norm5(self):
        rows = self.r3

        def piece(col, half):
            cube = self.apply(2 * col + half, rows, self.scale[half], self.shift[half])
            self.y3[col + 1, half, 1:rows + 1] = cube.astype(BF16)
            self.y3[col + 1, half, 0] = down_strip(cube[rows - 1]).astype(BF16)
            self.y3[col + 1, half, rows + 1] = up_strip(cube[0]).astype(BF16)

        return [functools.partial(piece, col, half) for col in range(self.cols // 8) for half in range(2)]

    def norm6(self):
        rows = self.r3
        row_parts = self.out.shape[0] // (self.cols // 8)
        per = STRIPS // row_parts

        def piece(col, half):
            for strip in range(STRIPS):
                part = self.acc[2 * col + half, pl.ds(strip, rows, stride=STRIPS), :]
                part = jnp.maximum(part * self.scale[half] + self.shift[half], 0.0)
                self.out[col * row_parts + strip // per, pl.ds((strip % per) * rows, rows), pl.ds(half * LANES, LANES)] = part.astype(BF16)

        return [functools.partial(piece, col, half) for col in range(self.cols // 8) for half in range(2)]

    def convs(self):
        return [self.conv1, self.conv2, self.conv3, self.conv4, self.conv5, self.conv6]

    def norms(self):
        return [self.norm1, self.norm2, self.norm3, self.norm4, self.norm5, self.norm6]


def load_image(stage_ref, image, x):
    quads = x.shape[0] - 1
    for quad in range(quads):
        row = stage_ref[image, pl.ds(quad, STRIPS, stride=quads), :]
        x[quad + 1] = row.astype(BF16)
        if quad == quads - 1:
            x[0] = down_strip(row).astype(BF16)


def zero_borders(z1, y2, z2, y3):
    z1[0] = jnp.zeros(z1.shape[1:], BF16)
    y2[0] = jnp.zeros(y2.shape[1:], BF16)
    y2[y2.shape[0] - 1] = jnp.zeros(y2.shape[1:], BF16)
    z2[0] = jnp.zeros(z2.shape[1:], BF16)
    y3[0] = jnp.zeros(y3.shape[1:], BF16)
    y3[y3.shape[0] - 1] = jnp.zeros(y3.shape[1:], BF16)


MESH = pl.DeviceIdType.MESH


def pack(x_ref, perm, packed):
    pairs, _, tile_cols, rows = x_ref.shape
    quads = rows // 4
    shape = (2 * rows, 4 * 2 * quads)
    k, n = iota(shape, 0), iota(shape, 1)
    row, image = rem(k, rows), div(k, rows)
    hit = (rem(row, 4) == div(n, 2 * quads)) & (div(row, 4) == rem(n, quads)) & (image == rem(div(n, quads), 2))
    perm[...] = jnp.where(hit, 1.0, 0.0).astype(BF16)
    step = 32

    def one(chunk, _):
        at = pl.ds(chunk * step, step)
        left = jnp.concatenate([x_ref[at, m].astype(F32).reshape(step * tile_cols, rows) for m in range(2)], axis=1).astype(BF16)
        moved = jnp.dot(left, perm[...], preferred_element_type=F32).reshape(step, tile_cols, shape[1])
        moved = jnp.concatenate([moved[:, :, t * LANES:(t + 1) * LANES] for t in range(4)], axis=1)
        packed[at] = moved.astype(BF16)
        return 0

    lax.fori_loop(0, pairs // step, one, 0)


def kernel(rows_n, cols_n, x_ref, w1, v1, r1, u1, d2, v2, r2, u2, d3, v3, r3, u3, o_ref, perm, packed, landed, staged,
           m1, m2, m3, m4, acc, x, y1, z1, y2, z2, y3, out, in_send, in_recv, out_send, out_recv, out_own):
    devices = rows_n * cols_n
    my_row, my_col = lax.axis_index("h"), lax.axis_index("w")
    me = my_col * rows_n + my_row
    pair_n = landed.shape[0]
    cols = cols_n * x_ref.shape[2]

    def place(offset):
        other = lax.rem(me + offset, devices)
        return other, {"h": lax.rem(other, rows_n), "w": lax.div(other, rows_n)}

    barrier = pltpu.get_barrier_semaphore()

    def greet(offset, _):
        pl.semaphore_signal(barrier, inc=1, device_id=place(offset)[1], device_id_type=MESH)
        return 0

    lax.fori_loop(1, devices, greet, 0)
    pack(x_ref, perm, packed)
    pl.semaphore_wait(barrier, devices - 1)

    def send_pair(pair, _):
        pltpu.make_async_copy(packed.at[me * pair_n + pair], landed.at[pair, my_row, my_col], in_recv.at[pair]).start()

        def send(offset, _):
            other, coords = place(offset)
            pltpu.make_async_remote_copy(
                src_ref=packed.at[other * pair_n + pair], dst_ref=landed.at[pair, my_row, my_col], send_sem=in_send,
                recv_sem=in_recv.at[pair], device_id=coords, device_id_type=MESH).start()
            return 0

        lax.fori_loop(1, devices, send, 0)
        return 0

    lax.fori_loop(0, pair_n, send_pair, 0)
    build_weights(w1, r1, d2, r2, m1, m2, m3, m4, cols)
    zero_borders(z1, y2, z2, y3)

    def two(ref):
        row = ref[...]
        return jnp.concatenate([row, row], axis=1)

    affines = [two(v1), two(u1), v2[...], u2[...], v3[...], u3[...]]
    mats = [m1, m2, m3, m4, d3, r3]
    quads = staged.shape[1] // rows_n

    def sent(slot):
        part = out.at[slot, pl.ds(0, devices - 1)]
        pltpu.make_async_copy(part, part, out_send.at[slot]).wait()
        pltpu.make_async_copy(out.at[slot, 0], out.at[slot, 0], out_own.at[slot]).wait()

    def one_pair(pair, _):
        pltpu.make_async_copy(landed.at[pair], landed.at[pair], in_recv.at[pair]).wait()
        for row in range(rows_n):
            turned = jnp.transpose(landed[pair, row].astype(F32).reshape(LANES, LANES))
            for m in range(2):
                staged[m, pl.ds(row * quads, quads)] = turned[m * quads:(m + 1) * quads]

        def one_image(m, _):
            load_image(staged, m, x)
            stream = Stream(mats, affines, acc, x, y1, z1, y2, z2, y3, out.at[m], cols)
            for layer in range(6):
                for piece in stream.convs()[layer]():
                    piece()
                stream.stats(layer)
                if layer == 5:
                    pl.when(pair > 0)(lambda: sent(m))
                for piece in stream.norms()[layer]():
                    piece()
            image = (me * pair_n + pair) * 2 + m
            pltpu.make_async_copy(out.at[m, me], o_ref.at[image], out_own.at[m]).start()

            def send(offset, _):
                other, coords = place(offset)
                pltpu.make_async_remote_copy(
                    src_ref=out.at[m, other], dst_ref=o_ref.at[image], send_sem=out_send.at[m], recv_sem=out_recv,
                    device_id=coords, device_id_type=MESH).start()
                return 0

            lax.fori_loop(1, devices, send, 0)
            return 0

        lax.fori_loop(0, 2, one_image, 0)
        return 0

    lax.fori_loop(0, pair_n, one_pair, 0)
    part = packed.at[pl.ds(0, pair_n * (devices - 1))]
    pltpu.make_async_copy(part, part, in_send).wait()
    sent(0)
    sent(1)
    part = o_ref.at[pl.ds(0, 2 * pair_n * (devices - 1))]
    pltpu.make_async_copy(part, part, out_recv).wait()


def solution(mesh):
    rows_n, cols_n = mesh.shape["h"], mesh.shape["w"]
    devices = rows_n * cols_n
    act_spec = P("batch", "h", "w")

    def local_forward(tile, *params):
        images, rows, tile_cols, _ = tile.shape
        cols = cols_n * tile_cols
        pairs = images // 2
        q = rows_n * rows // 4 // STRIPS
        blocks = cols // 4 + 1
        r2, r3 = q, q // 2
        x = jnp.transpose(tile, (0, 3, 2, 1)).reshape(pairs, 2, tile_cols, rows)
        flat = [param.reshape(-1, param.shape[-1]) for param in params]
        scratch = [
            pltpu.VMEM((2 * rows, 2 * rows), BF16),
            pltpu.VMEM((pairs, 4 * tile_cols, LANES), BF16),
            pltpu.VMEM((pairs // devices, rows_n, cols_n, 4 * tile_cols, LANES), BF16),
            pltpu.VMEM((2, q * STRIPS, LANES), F32),
            pltpu.VMEM((blocks, 2 * LANES, 2 * LANES), BF16),
            pltpu.VMEM((16 * 64, 2 * LANES), BF16),
            pltpu.VMEM((18 * 64, 2 * LANES), BF16),
            pltpu.VMEM((12 * LANES, 2 * LANES), BF16),
            pltpu.VMEM((2 * blocks, q * STRIPS, LANES), F32),
            pltpu.VMEM((q + 1, STRIPS, LANES), BF16),
            pltpu.VMEM((blocks, 2, q + 2, STRIPS, LANES), BF16),
            pltpu.VMEM((blocks, 2, q + 1, STRIPS, LANES), BF16),
            pltpu.VMEM((cols // 4 + 2, r2 + 2, STRIPS, LANES), BF16),
            pltpu.VMEM((cols // 4 + 1, 2, r3 + 1, STRIPS, LANES), BF16),
            pltpu.VMEM((cols // 8 + 2, 2, r3 + 2, STRIPS, LANES), BF16),
            pltpu.VMEM((2, devices, r3 * STRIPS // rows_n, 2 * LANES), BF16),
            pltpu.SemaphoreType.DMA,
            pltpu.SemaphoreType.DMA((pairs // devices,)),
            pltpu.SemaphoreType.DMA((2,)),
            pltpu.SemaphoreType.DMA,
            pltpu.SemaphoreType.DMA((2,)),
        ]
        out = pl.pallas_call(
            functools.partial(kernel, rows_n, cols_n),
            out_shape=jax.ShapeDtypeStruct((images, r3 * STRIPS // rows_n, 2 * LANES), BF16),
            in_specs=[pl.BlockSpec(memory_space=pltpu.VMEM)] * 13,
            out_specs=pl.BlockSpec(memory_space=pl.ANY),
            scratch_shapes=scratch,
            name="encoder",
            compiler_params=pltpu.CompilerParams(collective_id=0, has_side_effects=True, vmem_limit_bytes=56 * 1024 * 1024),
        )(x, *flat)
        return out.reshape(images, out.shape[1], 1, 2 * LANES)

    return jax.shard_map(local_forward, mesh=mesh, in_specs=(act_spec,) + (P(),) * 12, out_specs=act_spec, check_vma=False)
```

```python
import functools

import jax
import jax.numpy as jnp
from jax import lax
from jax.experimental import pallas as pl
from jax.experimental.pallas import tpu as pltpu
from jax.sharding import PartitionSpec as P

NORM_GROUPS = 8
NORM_EPS = 1e-5
F32 = jnp.float32
BF16 = jnp.bfloat16
LANES = 128
STRIPS = 16


def iota(shape, dim):
    return lax.broadcasted_iota(jnp.int32, shape, dim)


def div(value, by):
    return lax.div(value, jnp.int32(by))


def rem(value, by):
    return lax.rem(value, jnp.int32(by))


def blend(pieces, rows, cols):
    return jnp.concatenate([jnp.zeros((rows, cols), BF16) if piece is None else piece for piece in pieces], axis=1)


def tap(ref, depth, row, col):
    if 0 <= row < 3 and 0 <= col < 3:
        return ref[pl.ds((3 * row + col) * depth, depth), :]
    return None


def build_weights(w1_ref, r1_ref, d2_ref, r2_ref, m1, m2, m3, m4, cols):
    taps = [jnp.concatenate([w1_ref[t].astype(F32)] * 4, axis=1) for t in range(3)]
    shape = (2 * LANES, 2 * LANES)
    k, n = iota(shape, 0), iota(shape, 1)
    kk = rem(k, LANES)
    row = 4 * (div(k, LANES) - 1) + rem(div(kk, 8), 4)
    col = 8 * div(kk, 32) + rem(kk, 8)
    d_row = row - 2 * div(n, LANES) + 1
    half = rem(div(n, 64), 2)
    row_ok = (d_row >= 0) & (d_row < 3)

    def one_block(block, _):
        col_out = 2 * block - 1 + half
        d_col = col - 2 * col_out + 1
        good = row_ok & (d_col >= 0) & (d_col < 3) & (col_out >= 0) & (col_out < cols // 2)
        code = jnp.where(good, 3 * d_row + d_col, -1)
        total = jnp.zeros(shape, F32)
        for index in range(9):
            t, c = divmod(index, 3)
            total = jnp.where(code == index, taps[t][c:c + 1], total)
        m1[block] = total.astype(BF16)
        return 0

    lax.fori_loop(0, m1.shape[0], one_block, 0)
    for t in range(4):
        for q in range(4):
            m2[pl.ds((4 * t + q) * 64, 64), :] = blend([tap(r1_ref, 64, t - r, q - g) for r in range(2) for g in range(2)], 64, 64)
    for t in range(3):
        for q in range(6):
            m3[pl.ds((6 * t + q) * 64, 64), :] = blend([tap(d2_ref, 64, t, q - 1 - 2 * g) for g in range(2)], 64, LANES)
    for t in range(3):
        for q in range(4):
            m4[pl.ds((4 * t + q) * LANES, LANES), :] = blend([tap(r2_ref, LANES, t, q - g) for g in range(2)], LANES, LANES)


def group_matrix(period, group):
    shape = (LANES, LANES)
    return jnp.where(div(rem(iota(shape, 0), period), group) == div(rem(iota(shape, 1), period), group), 1.0, 0.0).astype(F32)


def relu16(value):
    return jnp.maximum(value, 0.0).astype(BF16)


def down_strip(row):
    return jnp.where(iota(row.shape, 0) == 0, 0.0, pltpu.roll(row, 1, 0))


def up_strip(row):
    return jnp.where(iota(row.shape, 0) == STRIPS - 1, 0.0, pltpu.roll(row, STRIPS - 1, 0))


def coefficients(sums, squares, folds, gamma, beta, count):
    both = jnp.concatenate([sums, squares], axis=0)
    both = jnp.dot(both, folds, preferred_element_type=F32, precision=lax.Precision.HIGHEST)
    total = jnp.sum(both[:STRIPS], axis=0, keepdims=True)
    total_sq = jnp.sum(both[STRIPS:], axis=0, keepdims=True)
    mean = total / count
    var = jnp.maximum(total_sq / count - jnp.square(mean), 0.0)
    inv = lax.rsqrt(var + NORM_EPS)
    scale = inv * gamma
    return scale, beta - mean * scale


class Stream:
    def __init__(self, mats, affines, acc, x, y1, z1, y2, z2, y3, out, cols):
        self.mats, self.affines = mats, affines
        self.acc, self.x, self.y1, self.z1, self.y2, self.z2, self.y3, self.out = acc, x, y1, z1, y2, z2, y3, out
        self.cols = cols
        self.q = x.shape[0] - 1
        self.r2 = y2.shape[1] - 2
        self.r3 = y3.shape[2] - 2
        self.sums = None
        self.squares = None
        self.gate = None

    def lhs(self, parts):
        parts = [part.reshape(part.shape[0] * STRIPS, LANES) for part in parts]
        return jnp.concatenate(parts, axis=1)

    def finish(self, summed, bias, first, second):
        rows = summed.shape[0]
        summed = summed + bias
        cube = summed.reshape(rows // STRIPS, STRIPS, 2 * LANES)
        square = cube * cube
        self.marks = square[:, :, :LANES]
        sums, squares = jnp.sum(cube, axis=0), jnp.sum(square, axis=0)
        self.sums = sums if self.sums is None else self.sums + sums
        self.squares = squares if self.squares is None else self.squares + squares
        self.acc[first, 0:rows] = summed[:, :LANES]
        self.acc[second, 0:rows] = summed[:, LANES:]

    def two(self, row):
        return jnp.concatenate([row, row], axis=1)

    def conv1(self):
        affine = self.affines[0]
        lane = iota((1, LANES), 1)
        blocks = self.mats[0].shape[0]
        bias = self.two(affine[0:1])

        def piece(block):
            own = bias
            if block == 0:
                own = self.two(jnp.where(lane < 64, 0.0, affine[0:1]))
            elif block == blocks - 1:
                own = self.two(jnp.where(lane < 64, affine[0:1], 0.0))
            left = self.lhs([self.x[0:self.q], self.x[1:self.q + 1]])
            self.finish(jnp.dot(left, self.mats[0][block], preferred_element_type=F32), own, 2 * block, 2 * block + 1)

        return [functools.partial(piece, block) for block in range(blocks)]

    def conv2(self):
        bias, q = self.two(self.affines[1][0:1]), self.q

        def piece(block):
            parts = []
            for parity, start in ((1, 0), (0, 1), (1, 1), (0, 2)):
                for near in range(2):
                    parts.append(self.y1[block + near, parity, start:start + q])
            self.finish(jnp.dot(self.lhs(parts), self.mats[1][...], preferred_element_type=F32), bias, 2 * block, 2 * block + 1)

        return [functools.partial(piece, block) for block in range(self.cols // 4)]

    def conv3(self):
        bias, q = self.two(self.affines[2][0:1]), self.q

        def piece(block):
            parts = []
            for parity, start in ((1, 0), (0, 1), (1, 1)):
                for near in range(3):
                    parts.append(self.z1[2 * block + near, parity, start:start + q])
            self.finish(jnp.dot(self.lhs(parts), self.mats[2][...], preferred_element_type=F32), bias, 2 * block, 2 * block + 1)

        return [functools.partial(piece, block) for block in range(self.cols // 8)]

    def conv4(self):
        bias = self.two(self.affines[3][0:1])

        def piece(block):
            parts = []
            for start in range(3):
                for near in range(4):
                    parts.append(self.y2[2 * block + near, start:start + self.r2])
            self.finish(jnp.dot(self.lhs(parts), self.mats[3][...], preferred_element_type=F32), bias, 2 * block, 2 * block + 1)

        return [functools.partial(piece, block) for block in range(self.cols // 8)]

    def conv5(self):
        bias = self.affines[4][0:1]

        def piece(col):
            parts = []
            for parity, start in ((1, 0), (0, 1), (1, 1)):
                for near in range(3):
                    parts.append(self.z2[2 * col + near, parity, start:start + self.r3])
            self.finish(jnp.dot(self.lhs(parts), self.mats[4][...], preferred_element_type=F32), bias, 2 * col, 2 * col + 1)

        return [functools.partial(piece, col) for col in range(self.cols // 8)]

    def conv6(self):
        bias = self.affines[5][0:1]

        def piece(col):
            parts = []
            for start in range(3):
                for near in range(3):
                    for half in range(2):
                        parts.append(self.y3[col + near, half, start:start + self.r3])
            self.finish(jnp.dot(self.lhs(parts), self.mats[5][...], preferred_element_type=F32), bias, 2 * col, 2 * col + 1)

        return [functools.partial(piece, col) for col in range(self.cols // 8)]

    def stats(self, layer):
        affine = self.affines[layer]
        period, group = ((64, 8), (LANES, 16), (LANES, 32))[layer // 2]
        folds = group_matrix(period, group)
        height = 1
        rows = (2 * self.q, self.r2, self.r3)[layer // 2]
        width = self.cols >> (layer // 2 + 1)
        count = float(height * rows * STRIPS * width * group)
        sums, squares = self.sums, self.squares
        self.sums = self.squares = None
        if layer < 4:
            sums, squares = sums[:, :LANES] + sums[:, LANES:], squares[:, :LANES] + squares[:, LANES:]
            self.scale, self.shift = coefficients(sums, squares, folds, affine[1:2], affine[2:3], count)
        else:
            pairs = [coefficients(sums[:, lo:lo + LANES], squares[:, lo:lo + LANES], folds, affine[1:2, lo:lo + LANES], affine[2:3, lo:lo + LANES], count) for lo in (0, LANES)]
            self.scale, self.shift = [pair[0] for pair in pairs], [pair[1] for pair in pairs]

    def due(self, scale, rows):
        if self.gate is None:
            return jnp.broadcast_to(scale, (rows, STRIPS, LANES))
        marks = self.gate
        have = marks.shape[0]
        if have > rows:
            marks = marks.reshape(rows, have // rows, STRIPS, LANES)[:, 0]
        elif have < rows:
            marks = jnp.broadcast_to(marks[:, None], (have, rows // have, STRIPS, LANES)).reshape(rows, STRIPS, LANES)
        return jnp.where(marks >= 0.0, scale, 0.0)

    def apply(self, block, rows, scale, shift):
        return self.acc[block, 0:rows * STRIPS].reshape(rows, STRIPS, LANES) * self.due(scale, rows) + shift

    def norm1(self):
        lane, q = iota((1, LANES), 1), self.q
        blocks = self.mats[0].shape[0]

        def piece(block, parity):
            scale, shift = self.scale, self.shift
            if block == 0:
                scale, shift = jnp.where(lane < 64, 0.0, scale), jnp.where(lane < 64, 0.0, shift)
            elif block == blocks - 1:
                scale, shift = jnp.where(lane < 64, scale, 0.0), jnp.where(lane < 64, shift, 0.0)
            cube = self.apply(2 * block + parity, q, scale, shift)
            self.y1[block, parity, 1:q + 1] = relu16(cube)
            if parity:
                self.y1[block, 1, 0] = relu16(down_strip(cube[q - 1]))
            else:
                self.y1[block, 0, q + 1] = relu16(up_strip(cube[0]))

        return [functools.partial(piece, block, parity) for block in range(blocks) for parity in range(2)]

    def norm2(self):
        q = self.q

        def piece(block, parity):
            cube = self.apply(2 * block + parity, q, self.scale, self.shift)
            self.z1[block + 1, parity, 1:q + 1] = relu16(cube)
            if parity:
                self.z1[block + 1, 1, 0] = relu16(down_strip(cube[q - 1]))

        return [functools.partial(piece, block, parity) for block in range(self.cols // 4) for parity in range(2)]

    def norm3(self):
        rows = self.r2

        def piece(col):
            cube = self.apply(col, rows, self.scale, self.shift)
            self.y2[col + 1, 1:rows + 1] = relu16(cube)
            self.y2[col + 1, 0] = relu16(down_strip(cube[rows - 1]))
            self.y2[col + 1, rows + 1] = relu16(up_strip(cube[0]))

        return [functools.partial(piece, col) for col in range(self.cols // 4)]

    def norm4(self):
        rows = self.r3

        def piece(col):
            cube = self.apply(col, 2 * rows, self.scale, self.shift).reshape(rows, 2, STRIPS, LANES)
            self.z2[col + 1, 0, 1:rows + 1] = relu16(cube[:, 0])
            self.z2[col + 1, 1, 1:rows + 1] = relu16(cube[:, 1])
            self.z2[col + 1, 1, 0] = relu16(down_strip(cube[rows - 1, 1]))

        return [functools.partial(piece, col) for col in range(self.cols // 4)]

    def norm5(self):
        rows = self.r3

        def piece(col, half):
            cube = self.apply(2 * col + half, rows, self.scale[half], self.shift[half])
            self.y3[col + 1, half, 1:rows + 1] = relu16(cube)
            self.y3[col + 1, half, 0] = relu16(down_strip(cube[rows - 1]))
            self.y3[col + 1, half, rows + 1] = relu16(up_strip(cube[0]))

        return [functools.partial(piece, col, half) for col in range(self.cols // 8) for half in range(2)]

    def norm6(self):
        rows = self.r3
        row_parts = self.out.shape[0] // (self.cols // 8)
        per = STRIPS // row_parts

        def piece(col, half):
            scale = self.due(self.scale[half], STRIPS)
            for strip in range(STRIPS):
                part = self.acc[2 * col + half, pl.ds(strip, rows, stride=STRIPS), :]
                part = part * scale[strip] + self.shift[half]
                self.out[col * row_parts + strip // per, pl.ds((strip % per) * rows, rows), pl.ds(half * LANES, LANES)] = relu16(part)

        return [functools.partial(piece, col, half) for col in range(self.cols // 8) for half in range(2)]

    def convs(self):
        return [self.conv1, self.conv2, self.conv3, self.conv4, self.conv5, self.conv6]

    def norms(self):
        return [self.norm1, self.norm2, self.norm3, self.norm4, self.norm5, self.norm6]


def weave(conv, convs, norm, norms):
    done = 0
    groups = max(len(convs) - 1, 1)
    for index, piece in enumerate(convs):
        piece()
        norm.gate = conv.marks
        upto = min(index + 1, groups) * len(norms) // groups
        for other in norms[done:upto]:
            other()
        done = upto
    norm.gate = None


def load_image(stage_ref, image, x):
    quads = x.shape[0] - 1

    def piece(quad):
        row = stage_ref[image, pl.ds(quad, STRIPS, stride=quads), :]
        x[quad + 1] = row.astype(BF16)
        if quad == quads - 1:
            x[0] = down_strip(row).astype(BF16)

    return [functools.partial(piece, quad) for quad in range(quads)]


def zero_borders(z1, y2, z2, y3):
    z1[0] = jnp.zeros(z1.shape[1:], BF16)
    y2[0] = jnp.zeros(y2.shape[1:], BF16)
    y2[y2.shape[0] - 1] = jnp.zeros(y2.shape[1:], BF16)
    z2[0] = jnp.zeros(z2.shape[1:], BF16)
    y3[0] = jnp.zeros(y3.shape[1:], BF16)
    y3[y3.shape[0] - 1] = jnp.zeros(y3.shape[1:], BF16)


MESH = pl.DeviceIdType.MESH


def pack(x_ref, perm, packed):
    pairs, _, tile_cols, rows = x_ref.shape
    quads = rows // 4
    shape = (2 * rows, 4 * 2 * quads)
    k, n = iota(shape, 0), iota(shape, 1)
    row, image = rem(k, rows), div(k, rows)
    hit = (rem(row, 4) == div(n, 2 * quads)) & (div(row, 4) == rem(n, quads)) & (image == rem(div(n, quads), 2))
    perm[...] = jnp.where(hit, 1.0, 0.0).astype(BF16)
    step = 32

    def one(chunk, _):
        at = pl.ds(chunk * step, step)
        left = jnp.concatenate([x_ref[at, m].astype(F32).reshape(step * tile_cols, rows) for m in range(2)], axis=1).astype(BF16)
        moved = jnp.dot(left, perm[...], preferred_element_type=F32).reshape(step, tile_cols, shape[1])
        moved = jnp.concatenate([moved[:, :, t * LANES:(t + 1) * LANES] for t in range(4)], axis=1)
        packed[at] = moved.astype(BF16)
        return 0

    lax.fori_loop(0, pairs // step, one, 0)


def kernel(rows_n, cols_n, x_ref, w1, v1, r1, u1, d2, v2, r2, u2, d3, v3, r3, u3, o_ref, perm, packed, landed, staged,
           m1, m2, m3, m4, acc, x, y1, z1, y2, z2, y3, out, in_send, in_recv, out_send, out_recv, out_own):
    devices = rows_n * cols_n
    my_row, my_col = lax.axis_index("h"), lax.axis_index("w")
    me = my_col * rows_n + my_row
    pair_n = landed.shape[0]
    cols = cols_n * x_ref.shape[2]

    def place(offset):
        other = lax.rem(me + offset, devices)
        return other, {"h": lax.rem(other, rows_n), "w": lax.div(other, rows_n)}

    barrier = pltpu.get_barrier_semaphore()

    def greet(offset, _):
        pl.semaphore_signal(barrier, inc=1, device_id=place(offset)[1], device_id_type=MESH)
        return 0

    lax.fori_loop(1, devices, greet, 0)
    pack(x_ref, perm, packed)
    pl.semaphore_wait(barrier, devices - 1)

    def send_pair(pair, _):
        pltpu.make_async_copy(packed.at[me * pair_n + pair], landed.at[pair, my_row, my_col], in_recv.at[pair]).start()

        def send(offset, _):
            other, coords = place(offset)
            pltpu.make_async_remote_copy(
                src_ref=packed.at[other * pair_n + pair], dst_ref=landed.at[pair, my_row, my_col], send_sem=in_send,
                recv_sem=in_recv.at[pair], device_id=coords, device_id_type=MESH).start()
            return 0

        lax.fori_loop(1, devices, send, 0)
        return 0

    lax.fori_loop(0, pair_n, send_pair, 0)
    build_weights(w1, r1, d2, r2, m1, m2, m3, m4, cols)
    for m in range(2):
        zero_borders(z1.at[m], y2.at[m], z2.at[m], y3.at[m])

    def two(ref):
        row = ref[...]
        return jnp.concatenate([row, row], axis=1)

    affines = [two(v1), two(u1), v2[...], u2[...], v3[...], u3[...]]
    mats = [m1, m2, m3, m4, d3, r3]
    quads = staged.shape[1] // rows_n

    def sent(slot):
        part = out.at[slot, pl.ds(0, devices - 1)]
        pltpu.make_async_copy(part, part, out_send.at[slot]).wait()
        pltpu.make_async_copy(out.at[slot, 0], out.at[slot, 0], out_own.at[slot]).wait()

    def one_pair(pair, _):
        pltpu.make_async_copy(landed.at[pair], landed.at[pair], in_recv.at[pair]).wait()
        for row in range(rows_n):
            turned = jnp.transpose(landed[pair, row].astype(F32).reshape(LANES, LANES))
            for m in range(2):
                staged[m, pl.ds(row * quads, quads)] = turned[m * quads:(m + 1) * quads]

        def streams(m):
            return Stream(mats, affines, acc.at[m], x.at[m], y1.at[m], z1.at[m], y2.at[m], z2.at[m], y3.at[m], out.at[m], cols)

        def ship(m):
            image = (me * pair_n + pair) * 2 + m
            pltpu.make_async_copy(out.at[m, me], o_ref.at[image], out_own.at[m]).start()

            def send(offset, _):
                other, coords = place(offset)
                pltpu.make_async_remote_copy(
                    src_ref=out.at[m, other], dst_ref=o_ref.at[image], send_sem=out_send.at[m], recv_sem=out_recv,
                    device_id=coords, device_id_type=MESH).start()
                return 0

            lax.fori_loop(1, devices, send, 0)

        first, second = streams(0), streams(1)
        for piece in load_image(staged, 0, x.at[0]):
            piece()
        for layer in range(6):
            weave(first, first.convs()[layer](), second, second.norms()[layer - 1]() if layer else load_image(staged, 1, x.at[1]))
            first.stats(layer)
            if layer == 5:
                pl.when(pair > 0)(lambda: sent(0))
            weave(second, second.convs()[layer](), first, first.norms()[layer]())
            second.stats(layer)
        ship(0)
        pl.when(pair > 0)(lambda: sent(1))
        for piece in second.norms()[5]():
            piece()
        ship(1)
        return 0

    lax.fori_loop(0, pair_n, one_pair, 0)
    part = packed.at[pl.ds(0, pair_n * (devices - 1))]
    pltpu.make_async_copy(part, part, in_send).wait()
    sent(0)
    sent(1)
    part = o_ref.at[pl.ds(0, 2 * pair_n * (devices - 1))]
    pltpu.make_async_copy(part, part, out_recv).wait()


def solution(mesh):
    rows_n, cols_n = mesh.shape["h"], mesh.shape["w"]
    devices = rows_n * cols_n
    act_spec = P("batch", "h", "w")

    def local_forward(tile, *params):
        images, rows, tile_cols, _ = tile.shape
        cols = cols_n * tile_cols
        pairs = images // 2
        q = rows_n * rows // 4 // STRIPS
        blocks = cols // 4 + 1
        r2, r3 = q, q // 2
        x = jnp.transpose(tile, (0, 3, 2, 1)).reshape(pairs, 2, tile_cols, rows)
        flat = [jnp.transpose(params[0], (0, 2, 1, 3)).reshape(3, 3, -1)]
        flat += [param.reshape(-1, param.shape[-1]) for param in params[1:]]
        scratch = [
            pltpu.VMEM((2 * rows, 2 * rows), BF16),
            pltpu.VMEM((pairs, 4 * tile_cols, LANES), BF16),
            pltpu.VMEM((pairs // devices, rows_n, cols_n, 4 * tile_cols, LANES), BF16),
            pltpu.VMEM((2, q * STRIPS, LANES), F32),
            pltpu.VMEM((blocks, 2 * LANES, 2 * LANES), BF16),
            pltpu.VMEM((16 * 64, 2 * LANES), BF16),
            pltpu.VMEM((18 * 64, 2 * LANES), BF16),
            pltpu.VMEM((12 * LANES, 2 * LANES), BF16),
            pltpu.VMEM((2, 2 * blocks, q * STRIPS, LANES), F32),
            pltpu.VMEM((2, q + 1, STRIPS, LANES), BF16),
            pltpu.VMEM((2, blocks, 2, q + 2, STRIPS, LANES), BF16),
            pltpu.VMEM((2, blocks, 2, q + 1, STRIPS, LANES), BF16),
            pltpu.VMEM((2, cols // 4 + 2, r2 + 2, STRIPS, LANES), BF16),
            pltpu.VMEM((2, cols // 4 + 1, 2, r3 + 1, STRIPS, LANES), BF16),
            pltpu.VMEM((2, cols // 8 + 2, 2, r3 + 2, STRIPS, LANES), BF16),
            pltpu.VMEM((2, devices, r3 * STRIPS // rows_n, 2 * LANES), BF16),
            pltpu.SemaphoreType.DMA,
            pltpu.SemaphoreType.DMA((pairs // devices,)),
            pltpu.SemaphoreType.DMA((2,)),
            pltpu.SemaphoreType.DMA,
            pltpu.SemaphoreType.DMA((2,)),
        ]
        out = pl.pallas_call(
            functools.partial(kernel, rows_n, cols_n),
            out_shape=pltpu.VMEM((images, r3 * STRIPS // rows_n, 2 * LANES), BF16),
            in_specs=[pl.BlockSpec(memory_space=pltpu.VMEM)] * 13,
            out_specs=pl.BlockSpec(memory_space=pl.ANY),
            scratch_shapes=scratch,
            name="encoder",
            compiler_params=pltpu.CompilerParams(collective_id=0, has_side_effects=True, vmem_limit_bytes=59 * 1024 * 1024 + 900 * 1024),
        )(x, *flat)
        return out.reshape(images, out.shape[1], 1, 2 * LANES)

    return jax.shard_map(local_forward, mesh=mesh, in_specs=(act_spec,) + (P(),) * 12, out_specs=act_spec, check_vma=False)
```

```python
import functools

import jax
import jax.numpy as jnp
from jax import lax
from jax.experimental import pallas as pl
from jax.experimental.pallas import tpu as pltpu
from jax.sharding import PartitionSpec as P

NORM_GROUPS = 8
NORM_EPS = 1e-5
F32 = jnp.float32
BF16 = jnp.bfloat16
LANES = 128
STRIPS = 16
SUB = 8
WAIT = 1
SPLIT = (1, 2, 4, 2, 2, 1)


def iota(shape, dim):
    return lax.broadcasted_iota(jnp.int32, shape, dim)


def div(value, by):
    return lax.div(value, jnp.int32(by))


def rem(value, by):
    return lax.rem(value, jnp.int32(by))


def blend(pieces, rows, cols):
    return jnp.concatenate([jnp.zeros((rows, cols), BF16) if piece is None else piece for piece in pieces], axis=1)


def tap(ref, depth, row, col):
    if 0 <= row < 3 and 0 <= col < 3:
        return ref[pl.ds((3 * row + col) * depth, depth), :]
    return None


def build_weights(w1_ref, r1_ref, d2_ref, r2_ref, m1, m2, m3, m4, cols):
    taps = [jnp.concatenate([w1_ref[t].astype(F32)] * 4, axis=1) for t in range(3)]
    shape = (2 * LANES, 2 * LANES)
    k, n = iota(shape, 0), iota(shape, 1)
    kk = rem(k, LANES)
    row = 4 * (div(k, LANES) - 1) + rem(div(kk, 8), 4)
    col = 8 * div(kk, 32) + rem(kk, 8)
    d_row = row - 2 * div(n, LANES) + 1
    half = rem(div(n, 64), 2)
    row_ok = (d_row >= 0) & (d_row < 3)

    def one_block(block, _):
        col_out = 2 * block - 1 + half
        d_col = col - 2 * col_out + 1
        good = row_ok & (d_col >= 0) & (d_col < 3) & (col_out >= 0) & (col_out < cols // 2)
        code = jnp.where(good, 3 * d_row + d_col, -1)
        total = jnp.zeros(shape, F32)
        for index in range(9):
            t, c = divmod(index, 3)
            total = jnp.where(code == index, taps[t][c:c + 1], total)
        m1[block] = total.astype(BF16)
        return 0

    lax.fori_loop(0, m1.shape[0], one_block, 0)
    for t in range(4):
        for q in range(4):
            m2[pl.ds((4 * t + q) * 64, 64), :] = blend([tap(r1_ref, 64, t - r, q - g) for r in range(2) for g in range(2)], 64, 64)
    for t in range(3):
        for q in range(6):
            m3[pl.ds((6 * t + q) * 64, 64), :] = blend([tap(d2_ref, 64, t, q - 1 - 2 * g) for g in range(2)], 64, LANES)
    for t in range(3):
        for q in range(4):
            m4[pl.ds((4 * t + q) * LANES, LANES), :] = blend([tap(r2_ref, LANES, t, q - g) for g in range(2)], LANES, LANES)


def group_matrix(period, group):
    shape = (LANES, LANES)
    return jnp.where(div(rem(iota(shape, 0), period), group) == div(rem(iota(shape, 1), period), group), 1.0, 0.0).astype(F32)


def relu16(value):
    return jnp.maximum(value, 0.0).astype(BF16)


def down_strip(row):
    return jnp.where(iota(row.shape, 0) == 0, 0.0, pltpu.roll(row, 1, 0))


def up_strip(row):
    return jnp.where(iota(row.shape, 0) == STRIPS - 1, 0.0, pltpu.roll(row, STRIPS - 1, 0))


def coefficients(sums, squares, folds, gamma, beta, count):
    both = jnp.concatenate([sums, squares], axis=0)
    both = jnp.dot(both, folds, preferred_element_type=F32, precision=lax.Precision.HIGHEST)
    total = jnp.sum(both[:STRIPS], axis=0, keepdims=True)
    total_sq = jnp.sum(both[STRIPS:], axis=0, keepdims=True)
    mean = total / count
    var = jnp.maximum(total_sq / count - jnp.square(mean), 0.0)
    inv = lax.rsqrt(var + NORM_EPS)
    scale = inv * gamma
    return scale, beta - mean * scale


class Stream:
    def __init__(self, mats, affines, acc, x, y1, z1, y2, z2, y3, out, cols):
        self.mats, self.affines = mats, affines
        self.acc, self.x, self.y1, self.z1, self.y2, self.z2, self.y3, self.out = acc, x, y1, z1, y2, z2, y3, out
        self.cols = cols
        self.q = x.shape[0] - 1
        self.r2 = y2.shape[1] - 2
        self.r3 = y3.shape[2] - 2
        self.sums = None
        self.squares = None
        self.gate = None

    def lhs(self, parts):
        parts = [part.reshape(part.shape[0] * STRIPS, LANES) for part in parts]
        return jnp.concatenate(parts, axis=1)

    def finish(self, summed, bias, first, second, low=0, turned=False):
        rows = summed.shape[0]
        at = pl.ds(low * STRIPS, rows)
        summed = summed + bias
        cube = summed.reshape(rows // STRIPS, STRIPS, 2 * LANES)
        square = cube * cube
        self.marks = square[:, :, :LANES]
        sums, squares = jnp.sum(cube, axis=0), jnp.sum(square, axis=0)
        self.sums = sums if self.sums is None else self.sums + sums
        self.squares = squares if self.squares is None else self.squares + squares
        if turned:
            cube = summed.reshape(rows // STRIPS, STRIPS // SUB, SUB, 2 * LANES)
            half_rows = rows // STRIPS * SUB
            for part in range(STRIPS // SUB):
                flat = cube[:, part].reshape(half_rows, 2 * LANES)
                self.acc[first, pl.ds(part * half_rows, half_rows)] = flat[:, :LANES]
                self.acc[second, pl.ds(part * half_rows, half_rows)] = flat[:, LANES:]
            return
        self.acc[first, at] = summed[:, :LANES]
        self.acc[second, at] = summed[:, LANES:]

    def two(self, row):
        return jnp.concatenate([row, row], axis=1)

    def conv1(self):
        affine = self.affines[0]
        lane = iota((1, LANES), 1)
        blocks = self.mats[0].shape[0]
        bias = self.two(affine[0:1])

        def piece(block):
            own = bias
            if block == 0:
                own = self.two(jnp.where(lane < 64, 0.0, affine[0:1]))
            elif block == blocks - 1:
                own = self.two(jnp.where(lane < 64, affine[0:1], 0.0))
            left = self.lhs([self.x[0:self.q], self.x[1:self.q + 1]])
            self.finish(jnp.dot(left, self.mats[0][block], preferred_element_type=F32), own, 2 * block, 2 * block + 1)

        return [functools.partial(piece, block) for block in range(blocks)]

    def conv2(self):
        bias, q = self.two(self.affines[1][0:1]), self.q

        step = q // SPLIT[1]

        def piece(block, low):
            parts = []
            for parity, start in ((1, 0), (0, 1), (1, 1), (0, 2)):
                for near in range(2):
                    parts.append(self.y1[block + near, parity, start + low:start + low + step])
            self.finish(jnp.dot(self.lhs(parts), self.mats[1][...], preferred_element_type=F32), bias, 2 * block, 2 * block + 1, low)

        return [functools.partial(piece, block, low) for block in range(self.cols // 4) for low in range(0, q, step)]

    def conv3(self):
        bias, q = self.two(self.affines[2][0:1]), self.q

        step = q // SPLIT[2]

        def piece(block, low):
            parts = []
            for parity, start in ((1, 0), (0, 1), (1, 1)):
                for near in range(3):
                    parts.append(self.z1[2 * block + near, parity, start + low:start + low + step])
            self.finish(jnp.dot(self.lhs(parts), self.mats[2][...], preferred_element_type=F32), bias, 2 * block, 2 * block + 1, low)

        return [functools.partial(piece, block, low) for block in range(self.cols // 8) for low in range(0, q, step)]

    def conv4(self):
        bias = self.two(self.affines[3][0:1])

        step = self.r2 // SPLIT[3]

        def piece(block, low):
            parts = []
            for start in range(3):
                for near in range(4):
                    parts.append(self.y2[2 * block + near, start + low:start + low + step])
            self.finish(jnp.dot(self.lhs(parts), self.mats[3][...], preferred_element_type=F32), bias, 2 * block, 2 * block + 1, low)

        return [functools.partial(piece, block, low) for block in range(self.cols // 8) for low in range(0, self.r2, step)]

    def conv5(self):
        bias = self.affines[4][0:1]

        step = self.r3 // SPLIT[4]

        def piece(col, low):
            parts = []
            for parity, start in ((1, 0), (0, 1), (1, 1)):
                for near in range(3):
                    parts.append(self.z2[2 * col + near, parity, start + low:start + low + step])
            self.finish(jnp.dot(self.lhs(parts), self.mats[4][...], preferred_element_type=F32), bias, 2 * col, 2 * col + 1, low)

        return [functools.partial(piece, col, low) for col in range(self.cols // 8) for low in range(0, self.r3, step)]

    def conv6(self):
        bias = self.affines[5][0:1]

        step = self.r3 // SPLIT[5]

        def piece(col, low):
            parts = []
            for start in range(3):
                for near in range(3):
                    for half in range(2):
                        parts.append(self.y3[col + near, half, start + low:start + low + step])
            self.finish(jnp.dot(self.lhs(parts), self.mats[5][...], preferred_element_type=F32), bias, 2 * col, 2 * col + 1, turned=True)

        return [functools.partial(piece, col, low) for col in range(self.cols // 8) for low in range(0, self.r3, step)]

    def stats(self, layer):
        affine = self.affines[layer]
        period, group = ((64, 8), (LANES, 16), (LANES, 32))[layer // 2]
        folds = group_matrix(period, group)
        height = 1
        rows = (2 * self.q, self.r2, self.r3)[layer // 2]
        width = self.cols >> (layer // 2 + 1)
        count = float(height * rows * STRIPS * width * group)
        sums, squares = self.sums, self.squares
        self.sums = self.squares = None
        if layer < 4:
            sums, squares = sums[:, :LANES] + sums[:, LANES:], squares[:, :LANES] + squares[:, LANES:]
            self.scale, self.shift = coefficients(sums, squares, folds, affine[1:2], affine[2:3], count)
        else:
            pairs = [coefficients(sums[:, lo:lo + LANES], squares[:, lo:lo + LANES], folds, affine[1:2, lo:lo + LANES], affine[2:3, lo:lo + LANES], count) for lo in (0, LANES)]
            self.scale, self.shift = [pair[0] for pair in pairs], [pair[1] for pair in pairs]

    def due(self, scale, rows):
        if self.gate is None:
            return jnp.broadcast_to(scale, (rows, STRIPS, LANES))
        marks = self.gate
        have = marks.shape[0]
        if have > rows:
            marks = marks.reshape(rows, have // rows, STRIPS, LANES)[:, 0]
        elif have < rows:
            marks = jnp.broadcast_to(marks[:, None], (have, rows // have, STRIPS, LANES)).reshape(rows, STRIPS, LANES)
        return jnp.where(marks >= 0.0, scale, 0.0)

    def apply(self, block, rows, scale, shift):
        return self.acc[block, 0:rows * STRIPS].reshape(rows, STRIPS, LANES) * self.due(scale, rows) + shift

    def norm1(self):
        lane, q = iota((1, LANES), 1), self.q
        blocks = self.mats[0].shape[0]

        def piece(block, parity):
            scale, shift = self.scale, self.shift
            if block == 0:
                scale, shift = jnp.where(lane < 64, 0.0, scale), jnp.where(lane < 64, 0.0, shift)
            elif block == blocks - 1:
                scale, shift = jnp.where(lane < 64, scale, 0.0), jnp.where(lane < 64, shift, 0.0)
            cube = self.apply(2 * block + parity, q, scale, shift)
            self.y1[block, parity, 1:q + 1] = relu16(cube)
            if parity:
                self.y1[block, 1, 0] = relu16(down_strip(cube[q - 1]))
            else:
                self.y1[block, 0, q + 1] = relu16(up_strip(cube[0]))

        return [functools.partial(piece, block, parity) for block in range(blocks) for parity in range(2)]

    def norm2(self):
        q = self.q

        def piece(block, parity):
            cube = self.apply(2 * block + parity, q, self.scale, self.shift)
            self.z1[block + 1, parity, 1:q + 1] = relu16(cube)
            if parity:
                self.z1[block + 1, 1, 0] = relu16(down_strip(cube[q - 1]))

        return [functools.partial(piece, block, parity) for block in range(self.cols // 4) for parity in range(2)]

    def norm3(self):
        rows = self.r2

        def piece(col):
            cube = self.apply(col, rows, self.scale, self.shift)
            self.y2[col + 1, 1:rows + 1] = relu16(cube)
            self.y2[col + 1, 0] = relu16(down_strip(cube[rows - 1]))
            self.y2[col + 1, rows + 1] = relu16(up_strip(cube[0]))

        return [functools.partial(piece, col) for col in range(self.cols // 4)]

    def norm4(self):
        rows = self.r3

        def piece(col):
            cube = self.apply(col, 2 * rows, self.scale, self.shift).reshape(rows, 2, STRIPS, LANES)
            self.z2[col + 1, 0, 1:rows + 1] = relu16(cube[:, 0])
            self.z2[col + 1, 1, 1:rows + 1] = relu16(cube[:, 1])
            self.z2[col + 1, 1, 0] = relu16(down_strip(cube[rows - 1, 1]))

        return [functools.partial(piece, col) for col in range(self.cols // 4)]

    def norm5(self):
        rows = self.r3

        def piece(col, half):
            cube = self.apply(2 * col + half, rows, self.scale[half], self.shift[half])
            self.y3[col + 1, half, 1:rows + 1] = relu16(cube)
            self.y3[col + 1, half, 0] = relu16(down_strip(cube[rows - 1]))
            self.y3[col + 1, half, rows + 1] = relu16(up_strip(cube[0]))

        return [functools.partial(piece, col, half) for col in range(self.cols // 8) for half in range(2)]

    def norm6(self):
        rows = self.r3
        row_parts = self.out.shape[0] // (self.cols // 8)
        per = STRIPS // row_parts

        def piece(col, half):
            scale = self.due(self.scale[half], STRIPS)
            for strip in range(STRIPS):
                part = self.acc[2 * col + half, pl.ds(strip // SUB * rows * SUB + strip % SUB, rows, stride=SUB), :]
                part = part * scale[strip] + self.shift[half]
                self.out[col * row_parts + strip // per, pl.ds((strip % per) * rows, rows), pl.ds(half * LANES, LANES)] = relu16(part)

        return [functools.partial(piece, col, half) for col in range(self.cols // 8) for half in range(2)]

    def convs(self):
        return [self.conv1, self.conv2, self.conv3, self.conv4, self.conv5, self.conv6]

    def norms(self):
        return [self.norm1, self.norm2, self.norm3, self.norm4, self.norm5, self.norm6]


def weave(conv, convs, norm, norms, prepare=None):
    done = 0
    start = min(WAIT, max(len(convs) - 3, 0))
    groups = max(len(convs) - 1 - start, 1)
    for index, piece in enumerate(convs):
        piece()
        if index < start:
            continue
        if index == start and prepare is not None:
            prepare()
        norm.gate = conv.marks
        upto = min(index - start + 1, groups) * len(norms) // groups
        for other in norms[done:upto]:
            other()
        done = upto
    norm.gate = None


def load_image(stage_ref, image, x):
    quads = x.shape[0] - 1

    def piece(quad):
        row = stage_ref[image, pl.ds(quad // SUB * STRIPS * SUB + quad % SUB, STRIPS, stride=SUB), :]
        x[quad + 1] = row.astype(BF16)
        if quad == quads - 1:
            x[0] = down_strip(row).astype(BF16)

    return [functools.partial(piece, quad) for quad in range(quads)]


def zero_borders(z1, y2, z2, y3):
    z1[0] = jnp.zeros(z1.shape[1:], BF16)
    y2[0] = jnp.zeros(y2.shape[1:], BF16)
    y2[y2.shape[0] - 1] = jnp.zeros(y2.shape[1:], BF16)
    z2[0] = jnp.zeros(z2.shape[1:], BF16)
    y3[0] = jnp.zeros(y3.shape[1:], BF16)
    y3[y3.shape[0] - 1] = jnp.zeros(y3.shape[1:], BF16)


MESH = pl.DeviceIdType.MESH


def pack(x_ref, perm, packed):
    pairs, _, tile_cols, rows = x_ref.shape
    quads = rows // 4
    shape = (2 * rows, 4 * 2 * quads)
    k, n = iota(shape, 0), iota(shape, 1)
    row, image = rem(k, rows), div(k, rows)
    hit = (rem(row, 4) == div(n, 2 * quads)) & (div(row, 4) == rem(n, quads)) & (image == rem(div(n, quads), 2))
    perm[...] = jnp.where(hit, 1.0, 0.0).astype(BF16)
    step = 32

    def one(chunk, _):
        at = pl.ds(chunk * step, step)
        left = jnp.concatenate([x_ref[at, m].astype(F32).reshape(step * tile_cols, rows) for m in range(2)], axis=1).astype(BF16)
        moved = jnp.dot(left, perm[...], preferred_element_type=F32).reshape(step, tile_cols, shape[1])
        moved = jnp.concatenate([moved[:, :, t * LANES:(t + 1) * LANES] for t in range(4)], axis=1)
        packed[at] = moved.astype(BF16)
        return 0

    lax.fori_loop(0, pairs // step, one, 0)


def kernel(rows_n, cols_n, x_ref, w1, v1, r1, u1, d2, v2, r2, u2, d3, v3, r3, u3, o_ref, perm, packed, landed, staged,
           m1, m2, m3, m4, acc, x, y1, z1, y2, z2, y3, out, in_send, in_recv, out_send, out_recv, out_own):
    devices = rows_n * cols_n
    my_row, my_col = lax.axis_index("h"), lax.axis_index("w")
    me = my_col * rows_n + my_row
    pair_n = landed.shape[0]
    cols = cols_n * x_ref.shape[2]

    def place(offset):
        other = lax.rem(me + offset, devices)
        return other, {"h": lax.rem(other, rows_n), "w": lax.div(other, rows_n)}

    barrier = pltpu.get_barrier_semaphore()

    def greet(offset, _):
        pl.semaphore_signal(barrier, inc=1, device_id=place(offset)[1], device_id_type=MESH)
        return 0

    lax.fori_loop(1, devices, greet, 0)
    pack(x_ref, perm, packed)
    pl.semaphore_wait(barrier, devices - 1)

    def send_pair(pair, _):
        pltpu.make_async_copy(packed.at[me * pair_n + pair], landed.at[pair, my_row, my_col], in_recv.at[pair]).start()

        def send(offset, _):
            other, coords = place(offset)
            pltpu.make_async_remote_copy(
                src_ref=packed.at[other * pair_n + pair], dst_ref=landed.at[pair, my_row, my_col], send_sem=in_send,
                recv_sem=in_recv.at[pair], device_id=coords, device_id_type=MESH).start()
            return 0

        lax.fori_loop(1, devices, send, 0)
        return 0

    lax.fori_loop(0, pair_n, send_pair, 0)
    build_weights(w1, r1, d2, r2, m1, m2, m3, m4, cols)
    for m in range(2):
        zero_borders(z1.at[m], y2.at[m], z2.at[m], y3.at[m])

    def two(ref):
        row = ref[...]
        return jnp.concatenate([row, row], axis=1)

    affines = [two(v1), two(u1), v2[...], u2[...], v3[...], u3[...]]
    mats = [m1, m2, m3, m4, d3, r3]
    quads, per_strip = staged.shape[1] // rows_n, staged.shape[1] // STRIPS

    def sent(slot):
        part = out.at[slot, pl.ds(0, devices - 1)]
        pltpu.make_async_copy(part, part, out_send.at[slot]).wait()
        pltpu.make_async_copy(out.at[slot, 0], out.at[slot, 0], out_own.at[slot]).wait()

    def one_pair(pair, _):
        pltpu.make_async_copy(landed.at[pair], landed.at[pair], in_recv.at[pair]).wait()
        for row in range(rows_n):
            turned = jnp.transpose(landed[pair, row].astype(F32).reshape(LANES, LANES))
            for m in range(2):
                for part in range(quads // SUB):
                    strip, eight = row * quads // per_strip + part * SUB // per_strip, part % (per_strip // SUB)
                    low = m * quads + part * SUB
                    staged[m, pl.ds((eight * STRIPS + strip) * SUB, SUB)] = turned[low:low + SUB]

        def streams(m):
            return Stream(mats, affines, acc.at[m], x.at[m], y1.at[m], z1.at[m], y2.at[m], z2.at[m], y3.at[m], out.at[m], cols)

        def ship(m):
            image = (me * pair_n + pair) * 2 + m
            pltpu.make_async_copy(out.at[m, me], o_ref.at[image], out_own.at[m]).start()

            def send(offset, _):
                other, coords = place(offset)
                pltpu.make_async_remote_copy(
                    src_ref=out.at[m, other], dst_ref=o_ref.at[image], send_sem=out_send.at[m], recv_sem=out_recv,
                    device_id=coords, device_id_type=MESH).start()
                return 0

            lax.fori_loop(1, devices, send, 0)

        first, second = streams(0), streams(1)
        for piece in load_image(staged, 0, x.at[0]):
            piece()
        for layer in range(6):
            if layer:
                weave(first, first.convs()[layer](), second, second.norms()[layer - 1](), functools.partial(second.stats, layer - 1))
            else:
                weave(first, first.convs()[0](), second, load_image(staged, 1, x.at[1]))
            if layer == 5:
                pl.when(pair > 0)(lambda: sent(0))
            weave(second, second.convs()[layer](), first, first.norms()[layer](), functools.partial(first.stats, layer))
        second.stats(5)
        ship(0)
        pl.when(pair > 0)(lambda: sent(1))
        for piece in second.norms()[5]():
            piece()
        ship(1)
        return 0

    lax.fori_loop(0, pair_n, one_pair, 0)
    part = packed.at[pl.ds(0, pair_n * (devices - 1))]
    pltpu.make_async_copy(part, part, in_send).wait()
    sent(0)
    sent(1)
    part = o_ref.at[pl.ds(0, 2 * pair_n * (devices - 1))]
    pltpu.make_async_copy(part, part, out_recv).wait()


def solution(mesh):
    rows_n, cols_n = mesh.shape["h"], mesh.shape["w"]
    devices = rows_n * cols_n
    act_spec = P("batch", "h", "w")

    def local_forward(tile, *params):
        images, rows, tile_cols, _ = tile.shape
        cols = cols_n * tile_cols
        pairs = images // 2
        q = rows_n * rows // 4 // STRIPS
        blocks = cols // 4 + 1
        r2, r3 = q, q // 2
        x = jnp.transpose(tile, (0, 3, 2, 1)).reshape(pairs, 2, tile_cols, rows)
        flat = [jnp.transpose(params[0], (0, 2, 1, 3)).reshape(3, 3, -1)]
        flat += [param.reshape(-1, param.shape[-1]) for param in params[1:]]
        scratch = [
            pltpu.VMEM((2 * rows, 2 * rows), BF16),
            pltpu.VMEM((pairs, 4 * tile_cols, LANES), BF16),
            pltpu.VMEM((pairs // devices, rows_n, cols_n, 4 * tile_cols, LANES), BF16),
            pltpu.VMEM((2, q * STRIPS, LANES), F32),
            pltpu.VMEM((blocks, 2 * LANES, 2 * LANES), BF16),
            pltpu.VMEM((16 * 64, 2 * LANES), BF16),
            pltpu.VMEM((18 * 64, 2 * LANES), BF16),
            pltpu.VMEM((12 * LANES, 2 * LANES), BF16),
            pltpu.VMEM((2, 2 * blocks, q * STRIPS, LANES), F32),
            pltpu.VMEM((2, q + 1, STRIPS, LANES), BF16),
            pltpu.VMEM((2, blocks, 2, q + 2, STRIPS, LANES), BF16),
            pltpu.VMEM((2, blocks, 2, q + 1, STRIPS, LANES), BF16),
            pltpu.VMEM((2, cols // 4 + 2, r2 + 2, STRIPS, LANES), BF16),
            pltpu.VMEM((2, cols // 4 + 1, 2, r3 + 1, STRIPS, LANES), BF16),
            pltpu.VMEM((2, cols // 8 + 2, 2, r3 + 2, STRIPS, LANES), BF16),
            pltpu.VMEM((2, devices, r3 * STRIPS // rows_n, 2 * LANES), BF16),
            pltpu.SemaphoreType.DMA,
            pltpu.SemaphoreType.DMA((pairs // devices,)),
            pltpu.SemaphoreType.DMA((2,)),
            pltpu.SemaphoreType.DMA,
            pltpu.SemaphoreType.DMA((2,)),
        ]
        out = pl.pallas_call(
            functools.partial(kernel, rows_n, cols_n),
            out_shape=pltpu.VMEM((images, r3 * STRIPS // rows_n, 2 * LANES), BF16),
            in_specs=[pl.BlockSpec(memory_space=pltpu.VMEM)] * 13,
            out_specs=pl.BlockSpec(memory_space=pl.ANY),
            scratch_shapes=scratch,
            name="encoder",
            compiler_params=pltpu.CompilerParams(collective_id=0, has_side_effects=True, vmem_limit_bytes=59 * 1024 * 1024 + 900 * 1024),
        )(x, *flat)
        return out.reshape(images, out.shape[1], 1, 2 * LANES)

    return jax.shard_map(local_forward, mesh=mesh, in_specs=(act_spec,) + (P(),) * 12, out_specs=act_spec, check_vma=False)
```

```python
import functools

import jax
import jax.numpy as jnp
from jax import lax
from jax.experimental import pallas as pl
from jax.experimental.pallas import tpu as pltpu
from jax.sharding import PartitionSpec as P

NORM_GROUPS = 8
NORM_EPS = 1e-5
F32 = jnp.float32
BF16 = jnp.bfloat16
LANES = 128
STRIPS = 16
SUB = 8
WIDE = 256
PHASES = ((1, 0), (0, 1), (1, 1))
WAIT = 1
SPLIT = (1, 2, 4, 2, 2, 1)


def iota(shape, dim):
    return lax.broadcasted_iota(jnp.int32, shape, dim)


def div(value, by):
    return lax.div(value, jnp.int32(by))


def rem(value, by):
    return lax.rem(value, jnp.int32(by))


def blend(pieces, rows, cols):
    return jnp.concatenate([jnp.zeros((rows, cols), BF16) if piece is None else piece for piece in pieces], axis=1)


def tap(ref, depth, row, col):
    if 0 <= row < 3 and 0 <= col < 3:
        return ref[pl.ds((3 * row + col) * depth, depth), :]
    return None


def build_weights(w1_ref, r1_ref, d2_ref, r2_ref, m1, m2, m3, m4, cols):
    taps = [jnp.concatenate([w1_ref[t].astype(F32)] * 4, axis=1) for t in range(3)]
    shape = (WIDE, WIDE)
    k, n = iota(shape, 0), iota(shape, 1)
    kk = rem(k, LANES)
    row = 4 * (div(k, LANES) - 1) + rem(div(kk, 8), 4)
    col = 8 * div(kk, 32) + rem(kk, 8)
    d_row = row - 2 * div(n, LANES) + 1
    half = rem(div(n, 64), 2)
    row_ok = (d_row >= 0) & (d_row < 3)

    def one_block(block, _):
        col_out = 2 * block - 1 + half
        d_col = col - 2 * col_out + 1
        good = row_ok & (d_col >= 0) & (d_col < 3) & (col_out >= 0) & (col_out < cols // 2)
        code = jnp.where(good, 3 * d_row + d_col, -1)
        total = jnp.zeros(shape, F32)
        for index in range(9):
            t, c = divmod(index, 3)
            total = jnp.where(code == index, taps[t][c:c + 1], total)
        m1[block] = total.astype(BF16)
        return 0

    lax.fori_loop(0, m1.shape[0], one_block, 0)
    for t in range(4):
        for q in range(4):
            m2[pl.ds((4 * t + q) * 64, 64), :] = blend([tap(r1_ref, 64, t - r, q - g) for r in range(2) for g in range(2)], 64, 64)
    for t in range(3):
        for q in range(6):
            m3[pl.ds((6 * t + q) * 64, 64), :] = blend([tap(d2_ref, 64, t, q - 1 - 2 * g) for g in range(2)], 64, LANES)
    for t in range(3):
        for q in range(4):
            m4[pl.ds((4 * t + q) * LANES, LANES), :] = blend([tap(r2_ref, LANES, t, q - g) for g in range(2)], LANES, LANES)


def group_matrix(period, group):
    shape = (LANES, LANES)
    return jnp.where(div(rem(iota(shape, 0), period), group) == div(rem(iota(shape, 1), period), group), 1.0, 0.0).astype(F32)


def relu16(value):
    return jnp.maximum(value, 0.0).astype(BF16)


def down_strip(row):
    return jnp.where(iota(row.shape, 0) == 0, 0.0, pltpu.roll(row, 1, 0))


def up_strip(row):
    return jnp.where(iota(row.shape, 0) == STRIPS - 1, 0.0, pltpu.roll(row, STRIPS - 1, 0))


def coefficients(sums, squares, folds, gamma, beta, count):
    both = jnp.concatenate([sums, squares], axis=0)
    both = jnp.dot(both, folds, preferred_element_type=F32, precision=lax.Precision.HIGHEST)
    total = jnp.sum(both[:STRIPS], axis=0, keepdims=True)
    total_sq = jnp.sum(both[STRIPS:], axis=0, keepdims=True)
    mean = total / count
    var = jnp.maximum(total_sq / count - jnp.square(mean), 0.0)
    inv = lax.rsqrt(var + NORM_EPS)
    scale = inv * gamma
    return scale, beta - mean * scale


class Stream:
    def __init__(self, mats, affines, acc, x, y1, z1, y2, z2, y3, out, cols):
        self.mats, self.affines = mats, affines
        self.acc, self.x, self.y1, self.z1, self.y2, self.z2, self.y3, self.out = acc, x, y1, z1, y2, z2, y3, out
        self.cols = cols
        self.q = x.shape[0] - 1
        self.r2 = y2.shape[1] - 2
        self.r3 = y3.shape[2] - 2
        self.sums = None
        self.squares = None
        self.gate = None

    def lhs(self, parts):
        parts = [part.reshape(part.shape[0] * STRIPS, LANES) for part in parts]
        return jnp.concatenate(parts, axis=1)

    def finish(self, summed, bias, first, second, low=0, turned=False):
        rows = summed.shape[0]
        at = pl.ds(low * STRIPS, rows)
        summed = summed + bias
        cube = summed.reshape(rows // STRIPS, STRIPS, WIDE)
        square = cube * cube
        self.marks = square[:, :, :LANES]
        sums, squares = jnp.sum(cube, axis=0), jnp.sum(square, axis=0)
        self.sums = sums if self.sums is None else self.sums + sums
        self.squares = squares if self.squares is None else self.squares + squares
        if turned:
            cube = summed.reshape(rows // STRIPS, STRIPS // SUB, SUB, WIDE)
            half_rows = rows // STRIPS * SUB
            for part in range(STRIPS // SUB):
                flat = cube[:, part].reshape(half_rows, WIDE)
                self.acc[first, pl.ds(part * half_rows, half_rows)] = flat[:, :LANES]
                self.acc[second, pl.ds(part * half_rows, half_rows)] = flat[:, LANES:]
            return
        self.acc[first, at] = summed[:, :LANES]
        self.acc[second, at] = summed[:, LANES:]

    def bias(self, layer):
        return self.affines[layer][0:1]

    def two(self, row):
        return jnp.concatenate([row, row], axis=1)

    def conv1(self):
        row = self.bias(0)
        lane = iota((1, LANES), 1)
        blocks = self.mats[0].shape[0]
        bias = self.two(row)

        def piece(block):
            own = bias
            if block == 0:
                own = self.two(jnp.where(lane < 64, 0.0, row))
            elif block == blocks - 1:
                own = self.two(jnp.where(lane < 64, row, 0.0))
            left = self.lhs([self.x[0:self.q], self.x[1:self.q + 1]])
            self.finish(jnp.dot(left, self.mats[0][block], preferred_element_type=F32), own, 2 * block, 2 * block + 1)

        return [functools.partial(piece, block) for block in range(blocks)]

    def conv2(self):
        bias, q = self.two(self.bias(1)), self.q

        step = q // SPLIT[1]

        def piece(block, low):
            parts = []
            for parity, start in PHASES + ((0, 2),):
                for near in range(2):
                    parts.append(self.y1[block + near, parity, start + low:start + low + step])
            self.finish(jnp.dot(self.lhs(parts), self.mats[1][...], preferred_element_type=F32), bias, 2 * block, 2 * block + 1, low)

        return [functools.partial(piece, block, low) for block in range(self.cols // 4) for low in range(0, q, step)]

    def conv3(self):
        bias, q = self.two(self.bias(2)), self.q

        step = q // SPLIT[2]

        def piece(block, low):
            parts = []
            for parity, start in PHASES:
                for near in range(3):
                    parts.append(self.z1[2 * block + near, parity, start + low:start + low + step])
            self.finish(jnp.dot(self.lhs(parts), self.mats[2][...], preferred_element_type=F32), bias, 2 * block, 2 * block + 1, low)

        return [functools.partial(piece, block, low) for block in range(self.cols // 8) for low in range(0, q, step)]

    def conv4(self):
        bias = self.two(self.bias(3))

        step = self.r2 // SPLIT[3]

        def piece(block, low):
            parts = []
            for start in range(3):
                for near in range(4):
                    parts.append(self.y2[2 * block + near, start + low:start + low + step])
            self.finish(jnp.dot(self.lhs(parts), self.mats[3][...], preferred_element_type=F32), bias, 2 * block, 2 * block + 1, low)

        return [functools.partial(piece, block, low) for block in range(self.cols // 8) for low in range(0, self.r2, step)]

    def conv5(self):
        bias = self.bias(4)

        step = self.r3 // SPLIT[4]

        def piece(col, low):
            parts = []
            for parity, start in PHASES:
                for near in range(3):
                    parts.append(self.z2[2 * col + near, parity, start + low:start + low + step])
            self.finish(jnp.dot(self.lhs(parts), self.mats[4][...], preferred_element_type=F32), bias, 2 * col, 2 * col + 1, low)

        return [functools.partial(piece, col, low) for col in range(self.cols // 8) for low in range(0, self.r3, step)]

    def conv6(self):
        bias = self.bias(5)

        step = self.r3 // SPLIT[5]

        def piece(col, low):
            parts = []
            for start in range(3):
                for near in range(3):
                    for half in range(2):
                        parts.append(self.y3[col + near, half, start + low:start + low + step])
            self.finish(jnp.dot(self.lhs(parts), self.mats[5][...], preferred_element_type=F32), bias, 2 * col, 2 * col + 1, turned=True)

        return [functools.partial(piece, col, low) for col in range(self.cols // 8) for low in range(0, self.r3, step)]

    def stats(self, layer):
        affine = self.affines[layer]
        period, group = ((64, 8), (LANES, 16), (LANES, 32))[layer // 2]
        folds = group_matrix(period, group)
        height = 1
        rows = (2 * self.q, self.r2, self.r3)[layer // 2]
        width = self.cols >> (layer // 2 + 1)
        count = float(height * rows * STRIPS * width * group)
        sums, squares = self.sums, self.squares
        self.sums = self.squares = None
        if layer < 4:
            sums, squares = sums[:, :LANES] + sums[:, LANES:], squares[:, :LANES] + squares[:, LANES:]
            self.scale, self.shift = coefficients(sums, squares, folds, affine[1:2], affine[2:3], count)
        else:
            pairs = [coefficients(sums[:, lo:lo + LANES], squares[:, lo:lo + LANES], folds, affine[1:2, lo:lo + LANES], affine[2:3, lo:lo + LANES], count) for lo in (0, LANES)]
            self.scale, self.shift = [pair[0] for pair in pairs], [pair[1] for pair in pairs]

    def due(self, scale, rows):
        if self.gate is None:
            return jnp.broadcast_to(scale, (rows, STRIPS, LANES))
        marks = self.gate
        have = marks.shape[0]
        if have > rows:
            marks = marks.reshape(rows, have // rows, STRIPS, LANES)[:, 0]
        elif have < rows:
            marks = jnp.broadcast_to(marks[:, None], (have, rows // have, STRIPS, LANES)).reshape(rows, STRIPS, LANES)
        return jnp.where(marks >= 0.0, scale, 0.0)

    def apply(self, block, rows, scale, shift):
        return self.acc[block, 0:rows * STRIPS].reshape(rows, STRIPS, LANES) * self.due(scale, rows) + shift

    def norm1(self):
        lane, q = iota((1, LANES), 1), self.q
        blocks = self.mats[0].shape[0]

        def piece(block, parity):
            scale, shift = self.scale, self.shift
            if block == 0:
                scale, shift = jnp.where(lane < 64, 0.0, scale), jnp.where(lane < 64, 0.0, shift)
            elif block == blocks - 1:
                scale, shift = jnp.where(lane < 64, scale, 0.0), jnp.where(lane < 64, shift, 0.0)
            cube = self.apply(2 * block + parity, q, scale, shift)
            self.y1[block, parity, 1:q + 1] = relu16(cube)
            if parity:
                self.y1[block, 1, 0] = relu16(down_strip(cube[q - 1]))
            else:
                self.y1[block, 0, q + 1] = relu16(up_strip(cube[0]))

        return [functools.partial(piece, block, parity) for block in range(blocks) for parity in range(2)]

    def norm2(self):
        q = self.q

        def piece(block, parity):
            cube = self.apply(2 * block + parity, q, self.scale, self.shift)
            self.z1[block + 1, parity, 1:q + 1] = relu16(cube)
            if parity:
                self.z1[block + 1, 1, 0] = relu16(down_strip(cube[q - 1]))

        return [functools.partial(piece, block, parity) for block in range(self.cols // 4) for parity in range(2)]

    def norm3(self):
        rows = self.r2

        def piece(col):
            cube = self.apply(col, rows, self.scale, self.shift)
            self.y2[col + 1, 1:rows + 1] = relu16(cube)
            self.y2[col + 1, 0] = relu16(down_strip(cube[rows - 1]))
            self.y2[col + 1, rows + 1] = relu16(up_strip(cube[0]))

        return [functools.partial(piece, col) for col in range(self.cols // 4)]

    def norm4(self):
        rows = self.r3

        def piece(col):
            cube = self.apply(col, 2 * rows, self.scale, self.shift).reshape(rows, 2, STRIPS, LANES)
            self.z2[col + 1, 0, 1:rows + 1] = relu16(cube[:, 0])
            self.z2[col + 1, 1, 1:rows + 1] = relu16(cube[:, 1])
            self.z2[col + 1, 1, 0] = relu16(down_strip(cube[rows - 1, 1]))

        return [functools.partial(piece, col) for col in range(self.cols // 4)]

    def norm5(self):
        rows = self.r3

        def piece(col, half):
            cube = self.apply(2 * col + half, rows, self.scale[half], self.shift[half])
            self.y3[col + 1, half, 1:rows + 1] = relu16(cube)
            self.y3[col + 1, half, 0] = relu16(down_strip(cube[rows - 1]))
            self.y3[col + 1, half, rows + 1] = relu16(up_strip(cube[0]))

        return [functools.partial(piece, col, half) for col in range(self.cols // 8) for half in range(2)]

    def norm6(self):
        rows = self.r3
        row_parts = self.out.shape[0] // (self.cols // 8)
        per = STRIPS // row_parts

        def piece(col, half):
            scale = self.due(self.scale[half], STRIPS)
            for strip in range(STRIPS):
                part = self.acc[2 * col + half, pl.ds(strip // SUB * rows * SUB + strip % SUB, rows, stride=SUB), :]
                part = part * scale[strip] + self.shift[half]
                self.out[col * row_parts + strip // per, pl.ds((strip % per) * rows, rows), pl.ds(half * LANES, LANES)] = relu16(part)

        return [functools.partial(piece, col, half) for col in range(self.cols // 8) for half in range(2)]

    def convs(self):
        return [self.conv1, self.conv2, self.conv3, self.conv4, self.conv5, self.conv6]

    def norms(self):
        return [self.norm1, self.norm2, self.norm3, self.norm4, self.norm5, self.norm6]


def weave(conv, convs, norm, norms, prepare=None):
    done = 0
    start = min(WAIT, max(len(convs) - 3, 0))
    groups = max(len(convs) - 1 - start, 1)
    for index, piece in enumerate(convs):
        piece()
        if index < start:
            continue
        if index == start and prepare is not None:
            prepare()
        norm.gate = conv.marks
        upto = min(index - start + 1, groups) * len(norms) // groups
        for other in norms[done:upto]:
            other()
        done = upto
    norm.gate = None


def load_image(stage_ref, image, x):
    quads = x.shape[0] - 1

    def piece(quad):
        row = stage_ref[image, pl.ds(quad // SUB * STRIPS * SUB + quad % SUB, STRIPS, stride=SUB), :]
        x[quad + 1] = row.astype(BF16)
        if quad == quads - 1:
            x[0] = down_strip(row).astype(BF16)

    return [functools.partial(piece, quad) for quad in range(quads)]


def zero_borders(z1, y2, z2, y3):
    z1[0] = jnp.zeros(z1.shape[1:], BF16)
    y2[0] = jnp.zeros(y2.shape[1:], BF16)
    y2[y2.shape[0] - 1] = jnp.zeros(y2.shape[1:], BF16)
    z2[0] = jnp.zeros(z2.shape[1:], BF16)
    y3[0] = jnp.zeros(y3.shape[1:], BF16)
    y3[y3.shape[0] - 1] = jnp.zeros(y3.shape[1:], BF16)


MESH = pl.DeviceIdType.MESH


def pack(x_ref, perm, packed):
    pairs, _, tile_cols, rows = x_ref.shape
    quads = rows // 4
    shape = (2 * rows, 4 * 2 * quads)
    k, n = iota(shape, 0), iota(shape, 1)
    row, image = rem(k, rows), div(k, rows)
    hit = (rem(row, 4) == div(n, 2 * quads)) & (div(row, 4) == rem(n, quads)) & (image == rem(div(n, quads), 2))
    perm[...] = jnp.where(hit, 1.0, 0.0).astype(BF16)
    step = 32

    def one(chunk, _):
        at = pl.ds(chunk * step, step)
        left = jnp.concatenate([x_ref[at, m].astype(F32).reshape(step * tile_cols, rows) for m in range(2)], axis=1).astype(BF16)
        moved = jnp.dot(left, perm[...], preferred_element_type=F32).reshape(step, tile_cols, shape[1])
        moved = jnp.concatenate([moved[:, :, t * LANES:(t + 1) * LANES] for t in range(4)], axis=1)
        packed[at] = moved.astype(BF16)
        return 0

    lax.fori_loop(0, pairs // step, one, 0)


def kernel(rows_n, cols_n, x_ref, w1, v1, r1, u1, d2, v2, r2, u2, d3, v3, r3, u3, o_ref, perm, packed, landed, staged,
           m1, m2, m3, m4, acc, x, y1, z1, y2, z2, y3, out, in_send, in_recv, out_send, out_recv, out_own, held, held_sem):
    devices = rows_n * cols_n
    my_row, my_col = lax.axis_index("h"), lax.axis_index("w")
    me = my_col * rows_n + my_row
    pair_n = landed.shape[0]
    cols = cols_n * x_ref.shape[2]

    def place(offset):
        other = lax.rem(me + offset, devices)
        return other, {"h": lax.rem(other, rows_n), "w": lax.div(other, rows_n)}

    barrier = pltpu.get_barrier_semaphore()

    def greet(offset, _):
        pl.semaphore_signal(barrier, inc=1, device_id=place(offset)[1], device_id_type=MESH)
        return 0

    lax.fori_loop(1, devices, greet, 0)
    loads = [pltpu.make_async_copy(ref, held[n], held_sem.at[n]) for n, ref in enumerate((r1, d2, r2, d3, r3))]
    for load in loads:
        load.start()
    pack(x_ref, perm, packed)
    pl.semaphore_wait(barrier, devices - 1)

    def send_pair(pair, _):
        pltpu.make_async_copy(packed.at[me * pair_n + pair], landed.at[pair, my_row, my_col], in_recv.at[pair]).start()

        def send(offset, _):
            other, coords = place(offset)
            pltpu.make_async_remote_copy(
                src_ref=packed.at[other * pair_n + pair], dst_ref=landed.at[pair, my_row, my_col], send_sem=in_send,
                recv_sem=in_recv.at[pair], device_id=coords, device_id_type=MESH).start()
            return 0

        lax.fori_loop(1, devices, send, 0)
        return 0

    lax.fori_loop(0, pair_n, send_pair, 0)
    for load in loads:
        load.wait()
    r1, d2, r2, d3, r3 = held
    build_weights(w1, r1, d2, r2, m1, m2, m3, m4, cols)
    for m in range(2):
        zero_borders(z1.at[m], y2.at[m], z2.at[m], y3.at[m])

    def two(ref):
        row = ref[...]
        return jnp.concatenate([row, row], axis=1)

    affines = [two(v1), two(u1), v2[...], u2[...], v3[...], u3[...]]
    mats = [m1, m2, m3, m4, d3, r3]
    quads, per_strip = staged.shape[1] // rows_n, staged.shape[1] // STRIPS

    def sent(slot):
        part = out.at[slot, pl.ds(0, devices - 1)]
        pltpu.make_async_copy(part, part, out_send.at[slot]).wait()
        pltpu.make_async_copy(out.at[slot, 0], out.at[slot, 0], out_own.at[slot]).wait()

    def one_pair(pair, _):
        pltpu.make_async_copy(landed.at[pair], landed.at[pair], in_recv.at[pair]).wait()
        for row in range(rows_n):
            turned = jnp.transpose(landed[pair, row].astype(F32).reshape(LANES, LANES))
            for m in range(2):
                for part in range(quads // SUB):
                    strip, eight = row * quads // per_strip + part * SUB // per_strip, part % (per_strip // SUB)
                    low = m * quads + part * SUB
                    staged[m, pl.ds((eight * STRIPS + strip) * SUB, SUB)] = turned[low:low + SUB]

        def streams(m):
            return Stream(mats, affines, acc.at[m], x.at[m], y1.at[m], z1.at[m], y2.at[m], z2.at[m], y3.at[m], out.at[m], cols)

        def ship(m):
            image = (me * pair_n + pair) * 2 + m
            pltpu.make_async_copy(out.at[m, me], o_ref.at[image], out_own.at[m]).start()

            def send(offset, _):
                other, coords = place(offset)
                pltpu.make_async_remote_copy(
                    src_ref=out.at[m, other], dst_ref=o_ref.at[image], send_sem=out_send.at[m], recv_sem=out_recv,
                    device_id=coords, device_id_type=MESH).start()
                return 0

            lax.fori_loop(1, devices, send, 0)

        first, second = streams(0), streams(1)
        for piece in load_image(staged, 0, x.at[0]):
            piece()
        for layer in range(6):
            if layer:
                weave(first, first.convs()[layer](), second, second.norms()[layer - 1](), functools.partial(second.stats, layer - 1))
            else:
                weave(first, first.convs()[0](), second, load_image(staged, 1, x.at[1]))
            if layer == 5:
                pl.when(pair > 0)(lambda: sent(0))
            weave(second, second.convs()[layer](), first, first.norms()[layer](), functools.partial(first.stats, layer))
        ship(0)
        second.stats(5)
        pl.when(pair > 0)(lambda: sent(1))
        for piece in second.norms()[5]():
            piece()
        ship(1)
        return 0

    lax.fori_loop(0, pair_n, one_pair, 0)
    part = packed.at[pl.ds(0, pair_n * (devices - 1))]
    pltpu.make_async_copy(part, part, in_send).wait()
    sent(0)
    sent(1)
    part = o_ref.at[pl.ds(0, 2 * pair_n * (devices - 1))]
    pltpu.make_async_copy(part, part, out_recv).wait()


def solution(mesh):
    rows_n, cols_n = mesh.shape["h"], mesh.shape["w"]
    devices = rows_n * cols_n
    act_spec = P("batch", "h", "w")

    def local_forward(tile, *params):
        images, rows, tile_cols, _ = tile.shape
        cols = cols_n * tile_cols
        pairs = images // 2
        q = rows_n * rows // 4 // STRIPS
        blocks = cols // 4 + 1
        r2, r3 = q, q // 2
        wide, narrow, rows3 = cols // 4, cols // 8, r3 * STRIPS // rows_n

        def both(*shape):
            return pltpu.VMEM((2, *shape), BF16)

        x = jnp.transpose(tile, (0, 3, 2, 1)).reshape(pairs, 2, tile_cols, rows)
        flat = [jnp.transpose(params[0], (0, 2, 1, 3)).reshape(3, 3, -1)]
        flat += [param.reshape(-1, param.shape[-1]) for param in params[1:]]
        large = (2, 4, 6, 8, 10)
        scratch = [
            pltpu.VMEM((2 * rows, 2 * rows), BF16),
            pltpu.VMEM((pairs, 4 * tile_cols, LANES), BF16),
            pltpu.VMEM((pairs // devices, rows_n, cols_n, 4 * tile_cols, LANES), BF16),
            pltpu.VMEM((2, q * STRIPS, LANES), F32),
            pltpu.VMEM((blocks, WIDE, WIDE), BF16),
            pltpu.VMEM((16 * 64, WIDE), BF16),
            pltpu.VMEM((18 * 64, WIDE), BF16),
            pltpu.VMEM((12 * LANES, WIDE), BF16),
            pltpu.VMEM((2, 2 * blocks, q * STRIPS, LANES), F32),
            both(q + 1, STRIPS, LANES),
            both(blocks, 2, q + 2, STRIPS, LANES),
            both(blocks, 2, q + 1, STRIPS, LANES),
            both(wide + 2, r2 + 2, STRIPS, LANES),
            both(wide + 1, 2, r3 + 1, STRIPS, LANES),
            both(narrow + 2, 2, r3 + 2, STRIPS, LANES),
            both(devices, rows3, WIDE),
            pltpu.SemaphoreType.DMA,
            pltpu.SemaphoreType.DMA((pairs // devices,)),
            pltpu.SemaphoreType.DMA((2,)),
            pltpu.SemaphoreType.DMA,
            pltpu.SemaphoreType.DMA((2,)),
            [pltpu.VMEM(flat[n].shape, BF16) for n in large],
            pltpu.SemaphoreType.DMA((len(large),)),
        ]
        out = pl.pallas_call(
            functools.partial(kernel, rows_n, cols_n),
            out_shape=pltpu.VMEM((images, rows3, WIDE), BF16),
            in_specs=[pl.BlockSpec(memory_space=pl.ANY if n - 1 in large else pltpu.VMEM) for n in range(len(flat) + 1)],
            out_specs=pl.BlockSpec(memory_space=pl.ANY),
            scratch_shapes=scratch,
            name="encoder",
            compiler_params=pltpu.CompilerParams(collective_id=0, has_side_effects=True, vmem_limit_bytes=59 * 1024 * 1024 + 900 * 1024),
        )(x, *flat)
        return out.reshape(images, out.shape[1], 1, WIDE)

    return jax.shard_map(local_forward, mesh=mesh, in_specs=(act_spec,) + (P(),) * 12, out_specs=act_spec, check_vma=False)
```
